32 devices in a mesh: section: 4 (over y, x), node: 4 (over z), torus: 2 (over core).
Axes of the slice: x: 2, y: 2, z: 4, core: 2. Of those that a mesh axis runs over, the one named last changes fastest.
Arguments:
- act_in: bfloat16 [4, 1024, 7168], P('section', 'node', 'torus'), may hold values from -28 to 28
- next_in: bfloat16 [1024, 7168], P('node', 'torus'), may hold values from -42 to 42
- routes: int32 [2, 4, 1024, 2], P(None, 'section', 'node'), may hold values from 0 to 3, all different within a row; in each aligned block of 256 rows (0 to 255, 256 to 511, ..., all dimensions but the last counted through in order) at most 160 rows name the same one
- route_w: float32 [2, 4, 1024, 2], P(None, 'section', 'node'), may hold values from 0.2 to 1
- hist: float32 [4], P('section'), may hold values from 2 to 8
- gate_w: bfloat16 [4, 4, 7168, 1024], P('section', 'node', 'torus'), may hold values from -0.0625 to 0.0625
- up_w: bfloat16 [4, 4, 7168, 1024], P('section', 'node', 'torus'), may hold values from -0.0625 to 0.0625
- down_w: bfloat16 [4, 4, 1024, 7168], P('section', 'node', None, 'torus'), may hold values from -0.09375 to 0.09375
Outputs:
- act_out: bfloat16 [2, 4, 1024, 7168], P(None, 'section', 'node', 'torus')
- peak_out: float32 [4, 2], P('section')
The draws below stay inside these ranges and needn't reach their ends.
Inputs may be any that keep to these rules, and one draw needn't show every extreme that they name: `routes`: each token names 2 different experts; within the 256 tokens of one index of node (aligned blocks of rows of one tick and layer) no expert is named more than 160 times, a bound that some block reaches.
All inputs are finite; a program needn't handle non-finite values.
Results may differ from the reference program's by a relative error of at most 0.012.
Values may be sent and summed in bfloat16 or wider, within the bound.
A program may use at most 128 MiB of HBM per device.

```python
import math
import jax
import jax.numpy as jnp
import numpy as np
from jax import lax

D = 7168
FFW = 1024
TOPK = 2
TICKS = 2
TOK_DEV = 256
SECTIONS = 4
EXPERTS = 4
CAP = 160
TOKENS = 1024
N_NODE = 4


def rising_rows(key, array_shape, factor):
    noise_key, scale_key = jax.random.split(key)
    rising = 1.0 + 2.0 * jnp.arange(TOKENS, dtype=jnp.float32) / TOKENS
    noise = jnp.clip(jax.random.normal(noise_key, array_shape, jnp.float32), -6.0, 6.0)
    spread = jnp.exp(jax.random.uniform(scale_key, array_shape[:-1] + (1,), jnp.float32, -0.7, 0.4))
    return (noise * spread * rising[:, None] * factor).astype(jnp.bfloat16)


def draw_act_in(key, part):
    return rising_rows(jax.random.fold_in(key, 11), (SECTIONS, TOKENS, D), 1.0)


def draw_next_in(key, part):
    return rising_rows(jax.random.fold_in(key, 23), (TOKENS, D), 1.5)


def levels(stream_key, dims, shards, low, top_value):
    level, own = 1.0, jax.random.fold_in(stream_key, 6)
    for axis_at, blocks in shards:
        steps = jnp.exp(jax.random.uniform(jax.random.fold_in(own, axis_at), (blocks,), jnp.float32, low / len(shards), top_value / len(shards)))
        level = level * jnp.repeat(steps, dims[axis_at] // blocks).reshape([-1 if axis == axis_at else 1 for axis in range(len(dims))])
    return level


def routed_block(own_key, own, number, rows, amount, top, reach, lean):
    order = jax.random.permutation(own_key, amount)
    heavy_load, ordinary = shares(amount, rows * top, reach, lean, True), shares(amount, rows * top, reach, lean, False)
    places = jnp.arange(amount)

    def named(tallies, turn):
        used = int((tallies > 0).sum())
        fixed = max(1, used // 4)
        shifted = fixed + (places - fixed + turn * (used - fixed)) % max(1, amount - fixed)
        return jnp.zeros((amount,), jnp.int32).at[order[jnp.where(places < fixed, places, shifted)]].set(jnp.asarray(tallies, jnp.int32))

    tallies = jnp.where(number % 4 == 0, named(heavy_load, number // 4), named(ordinary, number - number // 4 - 1))
    mixed = jax.random.permutation(jax.random.fold_in(own, 3), amount)
    source_of, sink = mixed[0:amount // 2 * 2:2], mixed[1:amount // 2 * 2:2]
    slack = jnp.minimum(tallies[source_of] - 1, reach - tallies[sink]) // 2
    slack = jnp.where((source_of == order[0]) | (sink == order[0]) | (tallies[sink] == 0), 0, jnp.maximum(slack, 0))
    shifted = jax.random.randint(jax.random.fold_in(own, 4), (amount // 2,), 0, 1 << 20) % (slack + 1)
    tallies = tallies.at[source_of].add(-shifted).at[sink].add(shifted)
    members = jnp.searchsorted(jnp.cumsum(tallies), jnp.arange(rows * top), side="right").astype(jnp.int32)
    grid = members.reshape(top, rows).T
    grid = grid[jax.random.permutation(jax.random.fold_in(own, 1), rows)]
    turn = jax.random.randint(jax.random.fold_in(own, 2), (rows, 1), 0, top)
    return jnp.take_along_axis(grid, (jnp.arange(top)[None, :] + turn) % top, axis=1)


def shares(count, total, limit, lean, full):
    portions = [(1 << 20) // math.isqrt(rank ** lean) + 1 for rank in range(1, count + 1)]
    largest = limit if full else min(limit, max(-(-total // count), total * portions[0] // sum(portions)))
    least = 1 if total - largest >= count - 1 else 0
    given, surplus = [largest] + [least] * (count - 1), total - largest - least * (count - 1)
    while surplus > 0:
        free = [i for i in range(1, count) if given[i] < largest] or [i for i in range(1, count) if given[i] < limit]
        pool, remaining = sum([portions[i] for i in free]), surplus
        for i in free:
            more = min(limit - given[i], max(1, remaining * portions[i] // pool), surplus)
            given[i] = given[i] + more
            surplus = surplus - more
    return np.array(given)


def bell_draw(stream_key, extent, scale, reach, cuts=(), held_as=jnp.bfloat16):
    values = scale * jax.random.normal(stream_key, extent, jnp.float32)
    if cuts:
        values = values * levels(stream_key, extent, cuts, -0.22, 0.18)
    return jnp.clip(values, -reach, reach).astype(held_as)


def setup_inputs(seed: int = 0) -> dict:
    key_of = jax.random.split(jax.random.key(seed), 9)
    act_in = draw_act_in(jax.random.fold_in(key_of[8], 71), 0)
    next_in = draw_next_in(jax.random.fold_in(key_of[8], 71), 0)
    routes_keys = jax.random.split(jax.random.fold_in(key_of[2], 1), TICKS * SECTIONS * TOKENS // TOK_DEV)
    routes_turns = jax.random.permutation(jax.random.fold_in(key_of[2], 3), TICKS * SECTIONS * TOKENS // TOK_DEV)
    routes = jax.vmap(lambda own, number: routed_block(jax.random.fold_in(key_of[2], 2), own, number, TOK_DEV, EXPERTS, TOPK, CAP, 2))(routes_keys, routes_turns).reshape((TICKS, SECTIONS, TOKENS, TOPK))
    route_w = jnp.clip(0.2 + 0.8 * jax.random.uniform(key_of[3], (TICKS, SECTIONS, TOKENS, TOPK), jnp.float32) ** levels(key_of[3], (TICKS, SECTIONS, TOKENS, TOPK), ((1, 4), (2, 4)), -0.2, 0.2), 0.2, 1.0)
    hist = jnp.clip(2.0 + 6.0 * jax.random.uniform(key_of[4], (SECTIONS,), jnp.float32) ** levels(key_of[4], (SECTIONS,), ((0, 4),), -0.2, 0.2), 2.0, 8.0)
    gate_w = bell_draw(key_of[5], (SECTIONS, EXPERTS, D, FFW), D ** -0.5, 0.0625, ((0, 4), (1, 4), (2, 2)))
    up_w = bell_draw(key_of[6], (SECTIONS, EXPERTS, D, FFW), D ** -0.5, 0.0625, ((0, 4), (1, 4), (2, 2)))
    down_w = bell_draw(key_of[7], (SECTIONS, EXPERTS, FFW, D), (4 * FFW) ** -0.5, 0.09375, ((0, 4), (1, 4), (3, 2)))
    return dict(act_in=act_in, next_in=next_in, routes=routes, route_w=route_w, hist=hist, gate_w=gate_w, up_w=up_w, down_w=down_w)


FP8_LIMIT = 448.0


def expert_rows(token_rows, gate_mat, up_mat, down_mat, dequant):
    gate_val = jnp.dot(token_rows, gate_mat, preferred_element_type=jnp.float32) * dequant
    up_val = jnp.dot(token_rows, up_mat, preferred_element_type=jnp.float32) * dequant
    hidden = (jax.nn.silu(gate_val) * up_val).astype(jnp.bfloat16)
    return jnp.dot(hidden, down_mat, preferred_element_type=jnp.float32).astype(jnp.bfloat16)


def moe_layer(stream, quant_scale, expert_of, weight_of, gate_all, up_all, down_all):
    quantized = jnp.clip(stream.astype(jnp.float32) * (FP8_LIMIT / quant_scale), -FP8_LIMIT, FP8_LIMIT).astype(jnp.bfloat16)
    dequant = quant_scale / FP8_LIMIT
    pair_count = TOKENS * TOPK
    flat_expert = expert_of.reshape(pair_count).astype(jnp.int32)
    flat_weight = weight_of.reshape(pair_count)
    slot_total = N_NODE * CAP
    positions = jnp.arange(pair_count, dtype=jnp.int32)

    def per_expert(expert_id):
        sort_keys = jnp.where(flat_expert == expert_id, positions, pair_count)
        chosen = jnp.argsort(sort_keys, stable=True)[:slot_total].astype(jnp.int32)
        is_valid = (flat_expert[chosen] == expert_id).astype(jnp.float32)
        token_ids = chosen // TOPK
        token_rows = quantized[token_ids]
        outputs = expert_rows(token_rows, gate_all[expert_id], up_all[expert_id], down_all[expert_id], dequant)
        return token_ids, outputs.astype(jnp.float32) * (flat_weight[chosen] * is_valid)[:, None]

    token_ids, contrib = lax.map(per_expert, jnp.arange(EXPERTS, dtype=jnp.int32))
    branch = jnp.zeros((TOKENS, D), jnp.float32).at[token_ids.reshape(-1)].add(contrib.reshape(-1, D))
    return (stream.astype(jnp.float32) + branch).astype(jnp.bfloat16)


def reference(act_in, next_in, routes, route_w, hist, gate_w, up_w, down_w):
    first_peaks = []
    first_tick = []
    for section_id in range(SECTIONS):
        stream = act_in[section_id]
        first_peaks.append(jnp.max(jnp.abs(stream.astype(jnp.float32))))
        first_tick.append(moe_layer(stream, hist[section_id], routes[0, section_id], route_w[0, section_id], gate_w[section_id], up_w[section_id], down_w[section_id]))
    second_peaks = []
    second_tick = []
    for section_id in range(SECTIONS):
        stream = next_in if section_id == 0 else first_tick[section_id - 1]
        second_peaks.append(jnp.max(jnp.abs(stream.astype(jnp.float32))))
        second_tick.append(moe_layer(stream, first_peaks[section_id], routes[1, section_id], route_w[1, section_id], gate_w[section_id], up_w[section_id], down_w[section_id]))
    act_out = jnp.stack([jnp.stack(first_tick), jnp.stack(second_tick)])
    peak_out = jnp.stack([jnp.stack(first_peaks), jnp.stack(second_peaks)], axis=1)
    return act_out, peak_out
```

```python
import functools

import jax
import jax.numpy as jnp
from jax import lax
from jax.experimental import pallas as pl
from jax.experimental.pallas import tpu as pltpu
from jax.sharding import PartitionSpec as P

FP8_LIMIT = 448.0
MAX_CHUNKS = 4
DEPTH = 2


def shifted(value, axis, steps):
    count = lax.axis_size(axis)
    return lax.ppermute(value, axis, [(i, (i + steps) % count) for i in range(count)])


def swapped(value, axis):
    count = lax.axis_size(axis)
    return lax.ppermute(value, axis, [(i, i ^ 1) for i in range(count)])


def to_next_section(value):
    count = lax.axis_size("section")
    return lax.ppermute(value, "section", [(i, i + 1) for i in range(count - 1)])


def dot(left, right):
    return lax.dot_general(left, right, (((1,), (0,)), ((), ())), preferred_element_type=jnp.float32)


def torus_sum(value):
    if lax.axis_size("torus") == 2:
        return value + swapped(value.astype(jnp.bfloat16), "torus").astype(jnp.float32)
    return lax.psum(value, "torus")


def after(value, *earlier):
    return lax.optimization_barrier((value, *earlier))[0]


def ring_max(value, axis):
    count = lax.axis_size(axis)
    if count & (count - 1):
        return lax.pmax(value, axis)
    step = 1
    while step < count:
        value = jnp.maximum(value, shifted(value, axis, step))
        step *= 2
    return value


def routing_tables(expert_of, weight_of, capacity, n_node, me):
    tokens = expert_of.shape[0]
    pair = jnp.stack([me, me ^ 1]).astype(jnp.float32)
    named = expert_of[:, None, :] == pair[None, :, None]
    hit = jnp.any(named, axis=2)
    wgt = jnp.sum(jnp.where(named, weight_of[:, None, :], 0.0), axis=2)
    earlier = (jnp.arange(tokens)[:, None] > jnp.arange(tokens)[None, :]).astype(jnp.bfloat16)
    slots = jnp.arange(capacity, dtype=jnp.float32)
    rank = dot(earlier, hit.astype(jnp.bfloat16))
    chosen = (rank[:, :, None] == slots) & hit[:, :, None]
    table = chosen.astype(jnp.bfloat16).reshape(tokens, 2 * capacity)
    combine = jnp.where(chosen, wgt[:, :, None], 0.0).astype(jnp.bfloat16)
    return table.T, combine.reshape(tokens, 2 * capacity)


def shards(act_in, next_in, routes, route_w, hist, gate_w, up_w, down_w):
    tokens = act_in.shape[1]
    ticks = routes.shape[0]
    top = routes.shape[3]
    n_node = lax.axis_size("node")
    groups = n_node // 2
    capacity = 5 * tokens * top // (4 * n_node)
    half = groups * capacity
    gate_mat, up_mat, down_mat = gate_w[0, 0], up_w[0, 0], down_w[0, 0]
    width = gate_mat.shape[0]
    count = max(c for c in range(1, MAX_CHUNKS + 1) if width % (128 * c) == 0)
    size = width // count
    me = lax.axis_index("node")
    section_now = lax.axis_index("section")

    own_peak = jnp.max(jnp.abs(act_in[0])).astype(jnp.float32)
    packed = jnp.concatenate(
        [routes.astype(jnp.float32).reshape(-1), route_w.reshape(-1), jnp.full((128,), own_peak)]
    )
    amount = ticks * tokens * top
    known = [packed] + [shifted(packed, "node", -2 * k) for k in range(1, groups)]
    tables = []
    for tick in range(ticks):
        pairs = []
        for info in known:
            expert_of = info[:amount].reshape(ticks, tokens, top)[tick]
            weight_of = info[amount : 2 * amount].reshape(ticks, tokens, top)[tick]
            pairs.append(routing_tables(expert_of, weight_of, capacity, n_node, me))
        tables.append(tuple(zip(*pairs)))

    cuts = [slice(c * size, (c + 1) * size) for c in range(count)]
    streams = [act_in[0][:, cut] for cut in cuts]
    scale = hist[0]
    first_peak = known[0][-1:]
    for info in known[1:]:
        first_peak = jnp.maximum(first_peak, info[-1:])
    first_peak = ring_max(first_peak, "torus")
    first_peak = jnp.maximum(first_peak, swapped(first_peak, "node"))
    outputs, peaks = [], [first_peak[0]]
    for tick in range(ticks):
        select, combine = tables[tick]
        if tick > 0:
            streams = [
                lax.optimization_barrier(
                    jnp.where(section_now == 0, next_in[:, cut], to_next_section(outputs[-1][c]))
                )
                for c, cut in enumerate(cuts)
            ]
            scale = peaks[tick - 1]
        factor = FP8_LIMIT / scale
        dequant = scale / FP8_LIMIT
        gate = up = None
        sent = []
        for c, cut in enumerate(cuts):
            quantized = jnp.clip(
                streams[c].astype(jnp.float32) * factor, -FP8_LIMIT, FP8_LIMIT
            ).astype(jnp.bfloat16)
            if c >= DEPTH:
                quantized = after(quantized, sent[c - DEPTH], first_peak)
            if tick > 0 and c == count - 1:
                seen = [after(s, sent[0]) if sent else s for s in streams]
                here = [jnp.max(jnp.abs(s)).astype(jnp.float32).reshape(1) for s in seen]
                here = jnp.max(jnp.concatenate(here), keepdims=True)
                here = ring_max(ring_max(here, "torus"), "node")
                peaks.append(here[0])
                quantized = after(quantized, here)
            elif tick == 0:
                quantized = after(quantized, known[-1])
            held = [quantized] + [shifted(quantized, "node", -2 * k) for k in range(1, groups)]
            picked = [dot(select[k], held[k]).astype(jnp.bfloat16) for k in range(groups)]
            mine = jnp.concatenate([p[:capacity] for p in picked], axis=0)
            sent.append(jnp.concatenate([p[capacity:] for p in picked], axis=0))
            rows = jnp.concatenate([mine, swapped(sent[c], "node")], axis=0)
            gate_part = dot(rows, gate_mat[cut])
            up_part = dot(rows, up_mat[cut])
            gate = gate_part if gate is None else gate + gate_part
            up = up_part if up is None else up + up_part
        gate = torus_sum(gate) * dequant
        up = torus_sum(up) * dequant
        hidden = (jax.nn.silu(gate) * up).astype(jnp.bfloat16)
        layer, crossed = [], []
        for c, cut in enumerate(cuts):
            away_rows = hidden[half:]
            if c >= DEPTH:
                away_rows = after(away_rows, crossed[c - DEPTH])
            away = dot(away_rows, down_mat[:, cut]).astype(jnp.bfloat16)
            home_rows = after(hidden[:half], away)
            home = dot(home_rows, down_mat[:, cut]).astype(jnp.bfloat16)
            back = swapped(away, "node")
            branch = None
            for k in reversed(range(groups)):
                span = slice(k * capacity, (k + 1) * capacity)
                part = dot(combine[k], jnp.concatenate([home[span], back[span]], axis=0))
                if k > 0:
                    part = part.astype(jnp.bfloat16)
                    crossed = crossed + [part] if k == groups - 1 else crossed
                    part = shifted(part, "node", 2 * k).astype(jnp.float32)
                branch = part if branch is None else branch + part
            layer.append((streams[c].astype(jnp.float32) + branch).astype(jnp.bfloat16))
        outputs.append(layer)
    act_out = jnp.stack([jnp.concatenate(layer, axis=1) for layer in outputs])
    return act_out[:, None], jnp.stack(peaks)[None, :]


MESH_ID = pl.DeviceIdType.MESH
CHUNKS = 4
OWN, TO_INNER, RELAY, PICKED, BACK, CROSS_OUT, CROSS_IN, HOME, NEXT, TORUS, KINDS = range(11)
TILE = 512


def routing_rows(routes, route_w, experts, chunks):
    ticks, tokens, _ = routes.shape
    low, high = jnp.min(routes, axis=2), jnp.max(routes, axis=2)
    key = (low * experts + high) * tokens + jnp.arange(tokens)[None, :]
    place = jnp.sum((key[:, None, :] < key[:, :, None]).astype(jnp.int32), axis=2)
    span = tokens // chunks
    index = (place % chunks) * span + place // chunks
    at = index[:, None, :] == jnp.arange(tokens)[None, :, None]
    named = routes[:, :, :, None] == jnp.arange(experts)[None, None, None, :]
    weight = jnp.sum(jnp.where(named, route_w[:, :, :, None], 0.0), axis=2)
    both = jnp.concatenate([weight, jnp.any(named, axis=2).astype(jnp.float32)], axis=2)
    table = jnp.sum(jnp.where(at[:, :, :, None], both[:, None, :, :], 0.0), axis=2)
    table = table.reshape(ticks, chunks, span, 2 * experts).transpose(0, 1, 3, 2)
    table = jnp.pad(table, ((0, 0), (0, 0), (0, 0), (0, 128 - span)))
    index = jnp.broadcast_to(index[:, None, :].astype(jnp.float32), (ticks, 8, tokens))
    return table, index


def fused_kernel(
    sections, experts, act_hbm, next_hbm, table, index, hist, gate_hbm, up_hbm, down_hbm,
    out_hbm, peak_out,
    source, gate_mat, up_mat, down_mat, rows, stream, picked_out, cross_out, home_out,
    back_in, own_sum, cross_in, cross_own, torus_out, torus_in, partial, hidden, order,
    tables, index_prev, scale_tile, peak_own, peak_pair, peak_mate, peak_far,
    send, recv, load_sem, store_sem, table_send, table_recv, index_sem, mate_sem, far_send, far_recv,
):
    tokens, width = act_hbm.shape
    ffw = down_hbm.shape[0]
    span = tokens // CHUNKS
    pick = picked_out.shape[1]
    tiles = width // TILE
    section, node, torus = (lax.axis_index(a) for a in ("section", "node", "torus"))
    outer = (node == 0) | (node == 3)
    inner = jnp.logical_not(outer)
    side = node // 2
    mate = jnp.where(outer, 1 + side, 3 * side)
    facing = 2 - side
    far = 3 - 3 * side
    here_in, here_out = 1 + side, 3 * side
    f32, bf16 = jnp.float32, jnp.bfloat16

    def move(kind, c, src, dst, target):
        return pltpu.make_async_remote_copy(
            src_ref=src, dst_ref=dst, send_sem=send.at[kind, c], recv_sem=recv.at[kind, c],
            device_id=target, device_id_type=MESH_ID,
        )

    def at_node(n):
        return (section, n, torus)

    def part(c, first, count=1):
        return rows.at[c, pl.ds(first * span, count * span), :]

    def own_copy(c):
        return move(OWN, c, part(c, 1), part(c, 2), at_node(facing))

    def to_inner(c):
        return move(TO_INNER, c, part(c, 1), part(c, 0), at_node(mate))

    def relay(c):
        return move(RELAY, c, part(c, 0), part(c, 3), at_node(facing))

    def picked(c):
        return move(PICKED, c, picked_out.at[c % 2], part(c, 2, 2), at_node(mate))

    def back(c):
        return move(BACK, c, part(c, 2, 2), back_in.at[c], at_node(mate))

    def cross_to_outer(c):
        return move(CROSS_OUT, c, cross_out.at[c % 2, pl.ds(span, span), :], cross_in.at[c], at_node(facing))

    def cross_to_inner(c):
        return move(CROSS_IN, c, cross_out.at[c % 2, pl.ds(0, span), :], cross_own.at[c], at_node(facing))

    def home(c):
        return move(HOME, c, home_out.at[c % 2], cross_own.at[c], at_node(mate))

    def to_next(c):
        strip = pl.ds(c * span, span)
        return move(NEXT, c, stream.at[0, strip, :], source.at[1, strip, :], (section + 1, node, torus))

    def across(c):
        return move(TORUS, c, torus_out, torus_in.at[c % 2], (section, node, 1 - torus))

    def eye(count):
        return lax.broadcasted_iota(jnp.int32, (count, count), 0) == lax.broadcasted_iota(
            jnp.int32, (count, count), 1
        )

    def column(row):
        count = row.shape[1]
        return jnp.sum(jnp.where(eye(count), row, 0.0), axis=1, keepdims=True)

    def row_of(block, number):
        at = lax.broadcasted_iota(jnp.int32, block.shape, 0) == number
        return jnp.sum(jnp.where(at, block, 0.0), axis=0, keepdims=True)

    def spread(t, c):
        left = tables[here_out, t, c] + pltpu.roll(tables[here_in, t, c], span, 1)
        right = tables[facing, t, c] + pltpu.roll(tables[far, t, c], span, 1)
        return jnp.concatenate([left, right], axis=1)

    def outer_ranks(block):
        count = block.shape[1]
        lanes = lax.broadcasted_iota(jnp.int32, (1, count), 1)
        hit = jnp.where(lanes >= span, row_of(block, experts + here_out), 0.0)
        before = lax.broadcasted_iota(jnp.int32, (count, count), 0) < lax.broadcasted_iota(
            jnp.int32, (count, count), 1
        )
        wide = jnp.broadcast_to(hit, (8, count)).astype(bf16)
        rank = dot(wide, jnp.where(before, 1.0, 0.0).astype(bf16))[0:1]
        return jnp.where(hit > 0.0, rank, -1.0)

    def places(count, other, axis):
        return lax.broadcasted_iota(jnp.int32, (count, other), axis).astype(f32)

    def tile_at(k):
        return pl.ds(pl.multiple_of(k * TILE, TILE), TILE)

    def prepare(t, c):
        factor = FP8_LIMIT / scale_tile[0:1, 0:1]
        strip = pl.ds(pl.multiple_of(c * span, span), span)

        @pl.loop(0, tiles)
        def _(k):
            cols = tile_at(k)
            value = dot(order[strip, :], source[t, :, cols])
            stream[t, strip, cols] = value.astype(bf16)
            top = jnp.max(jnp.max(jnp.abs(value), axis=0, keepdims=True), axis=1, keepdims=True)
            peak_own[t] = jnp.maximum(peak_own[t], top)
            rows[c, pl.ds(span, span), cols] = jnp.clip(
                value * factor, -FP8_LIMIT, FP8_LIMIT
            ).astype(bf16)

    def select_for_outer(t, c):
        rank = outer_ranks(spread(t, c))
        table_mat = jnp.where(places(pick, tokens, 0) == rank, 1.0, 0.0).astype(bf16)

        @pl.loop(0, tiles)
        def _(k):
            cols = tile_at(k)
            picked_out[c % 2, :, cols] = dot(table_mat, rows[c, :, cols]).astype(bf16)

    def project(c):
        step = 256

        @pl.loop(0, ffw // step)
        def _(k):
            cols = pl.ds(pl.multiple_of(k * step, step), step)
            late = pl.ds(pl.multiple_of(ffw + k * step, step), step)
            value = dot(rows[c], gate_mat[:, cols])
            partial[:, cols] = value
            torus_out[:, cols] = value.astype(bf16)
            value = dot(rows[c], up_mat[:, cols])
            partial[:, late] = value
            torus_out[:, late] = value.astype(bf16)

    def activate(c):
        dequant = scale_tile[0:1, 0:1] / FP8_LIMIT
        step = 256

        @pl.loop(0, ffw // step)
        def _(k):
            cols = pl.ds(pl.multiple_of(k * step, step), step)
            late = pl.ds(pl.multiple_of(ffw + k * step, step), step)
            gate = (partial[:, cols] + torus_in[c % 2, :, cols].astype(f32)) * dequant
            up = (partial[:, late] + torus_in[c % 2, :, late].astype(f32)) * dequant
            hidden[:, cols] = (gate / (1.0 + jnp.exp(-gate)) * up).astype(bf16)

    def lower(c):
        @pl.loop(0, tiles)
        def _(k):
            cols = tile_at(k)
            rows[c, :, cols] = dot(hidden[...], down_mat[:, cols]).astype(bf16)

    def cross(t, c):
        block = spread(t, c)
        rank = column(outer_ranks(block))[span:]
        scatter = jnp.where(places(tokens - span, pick, 1) == rank, 1.0, 0.0).astype(bf16)
        weight_in = column(row_of(block, here_in))[span:]
        weight_out = column(row_of(block, here_out))[span:]

        @pl.loop(0, tiles)
        def _(k):
            cols = tile_at(k)
            value = weight_out * dot(scatter, back_in[c, :, cols])
            value = value + weight_in * rows[c, pl.ds(span, tokens - span), cols].astype(f32)
            own_sum[c % 2, :, cols] = value[:span]
            cross_out[c % 2, :, cols] = value[span:].astype(bf16)

    def bring_home(t, c):
        weight = column(row_of(tables[here_out, t, c], here_in))[:span]

        @pl.loop(0, tiles)
        def _(k):
            cols = tile_at(k)
            value = weight * rows[c, pl.ds(0, span), cols].astype(f32) + cross_in[c, :, cols].astype(f32)
            home_out[c % 2, :, cols] = value.astype(bf16)

    def own_part(t, c):
        weight = column(row_of(tables[node, t, c], node))[:span]

        @pl.loop(0, tiles)
        def _(k):
            cols = tile_at(k)
            own_sum[c % 2, :, cols] = weight * rows[c, pl.ds(span, span), cols].astype(f32)

    def finish(t, c):
        strip = pl.ds(pl.multiple_of(c * span, span), span)

        @pl.loop(0, tiles)
        def _(k):
            cols = tile_at(k)
            value = stream[t, strip, cols].astype(f32) + own_sum[c % 2, :, cols]
            stream[t, strip, cols] = (value + cross_own[c, :, cols].astype(f32)).astype(bf16)

    def store_copy(t, k):
        return pltpu.make_async_copy(source.at[t, :, tile_at(k)], out_hbm.at[t, :, tile_at(k)], store_sem.at[t, k])

    def write_out(t):
        spot = column(index[t][0:1])
        undo = jnp.where(places(tokens, tokens, 1) == spot, 1.0, 0.0).astype(bf16)

        @pl.loop(0, tiles)
        def _(k):
            cols = tile_at(k)
            source[t, :, cols] = dot(undo, stream[t, :, cols]).astype(bf16)
            store_copy(t, k).start()

    first_load = pltpu.make_async_copy(act_hbm, source.at[0], load_sem.at[0])
    first_load.start()
    next_load = pltpu.make_async_copy(next_hbm, source.at[1], load_sem.at[1])
    loads = [
        pltpu.make_async_copy(hbm, mat, load_sem.at[2 + i])
        for i, (hbm, mat) in enumerate(((gate_hbm, gate_mat), (up_hbm, up_mat), (down_hbm, down_mat)))
    ]
    tables[node] = table[...]
    table_copies = []
    for k in range(1, 4):
        other = lax.rem(node + k, 4)
        table_copies.append(
            pltpu.make_async_remote_copy(
                src_ref=table, dst_ref=tables.at[node], send_sem=table_send.at[k - 1],
                recv_sem=table_recv.at[node], device_id=at_node(other), device_id_type=MESH_ID,
            )
        )
    index_copy = pltpu.make_async_remote_copy(
        src_ref=index.at[0], dst_ref=index_prev, send_sem=index_sem.at[0], recv_sem=index_sem.at[1],
        device_id=(section + 1, node, torus), device_id_type=MESH_ID,
    )

    def mate_copy(t):
        return pltpu.make_async_remote_copy(
            src_ref=peak_own.at[t], dst_ref=peak_mate.at[t], send_sem=mate_sem.at[0, t],
            recv_sem=mate_sem.at[1, t], device_id=(section, node, 1 - torus), device_id_type=MESH_ID,
        )

    def far_copy(t, k):
        return pltpu.make_async_remote_copy(
            src_ref=peak_pair.at[t], dst_ref=peak_far.at[t, node], send_sem=far_send.at[t, k - 1],
            recv_sem=far_recv.at[t, node], device_id=at_node(lax.rem(node + k, 4)), device_id_type=MESH_ID,
        )

    scale_tile[...] = jnp.broadcast_to(hist[...], scale_tile.shape)
    peak_own[...] = jnp.zeros_like(peak_own)
    order[...] = jnp.where(places(tokens, tokens, 0) == index[0][0:1], 1.0, 0.0).astype(bf16)

    @pl.when(outer)
    def _():
        rows[:, 0:span, :] = jnp.zeros((CHUNKS, span, width), bf16)

    for copy in table_copies:
        copy.start()

    @pl.when(section < sections - 1)
    def _():
        index_copy.start()

    for copy in loads:
        copy.start()

    @pl.when(section == 0)
    def _():
        next_load.start()
        index_prev[...] = places(8, tokens, 1)

    first_load.wait()

    @pl.loop(0, 2)
    def _(t):
        @pl.when(t == 1)
        def _():
            @pl.when(section == 0)
            def _():
                next_load.wait()

            @pl.when(section > 0)
            def _():
                index_copy.wait_recv()

                @pl.loop(0, CHUNKS)
                def _(c):
                    to_next(c).wait_recv()

            now = jnp.where(places(tokens, tokens, 0) == index[1][0:1], 1.0, 0.0).astype(bf16)
            was = jnp.where(places(tokens, tokens, 0) == index_prev[0:1], 1.0, 0.0).astype(bf16)
            order[...] = lax.dot_general(
                now, was, (((1,), (1,)), ((), ())), preferred_element_type=f32
            ).astype(bf16)

        @pl.loop(0, jnp.where(outer, CHUNKS, 2))
        def _(c):
            prepare(t, c)

            @pl.when(outer)
            def _():
                to_inner(c).start()

            @pl.when(inner)
            def _():
                own_copy(c).start()

                @pl.when(c == 0)
                def _():
                    to_inner(0).wait_recv()
                    relay(0).start()

        @pl.when(t == 0)
        def _():
            for k in range(1, 4):
                other = lax.rem(node + k, 4)
                pltpu.make_async_remote_copy(
                    src_ref=table, dst_ref=tables.at[other], send_sem=table_send.at[k - 1],
                    recv_sem=table_recv.at[other], device_id=at_node(other), device_id_type=MESH_ID,
                ).wait_recv()

        @pl.when(t == 1)
        def _():
            write_out(0)

        @pl.loop(0, CHUNKS + 3)
        def _(it):
            @pl.when(it == 2)
            def _():
                mate_copy(t).start()

            @pl.when(it == 3)
            def _():
                mate_copy(t).wait_recv()
                peak_pair[t] = jnp.maximum(peak_own[t], peak_mate[t])
                for k in range(1, 4):
                    far_copy(t, k).start()

            @pl.when(it < CHUNKS)
            def _():
                @pl.when(inner)
                def _():
                    own_copy(it).wait_recv()
                    relay(it).wait_recv()

                    @pl.when(it >= 2)
                    def _():
                        picked(it - 2).wait_send()

                    select_for_outer(t, it)
                    picked(it).start()

                    @pl.when(it + 1 < CHUNKS)
                    def _():
                        to_inner(it + 1).wait_recv()
                        relay(it + 1).start()

                    @pl.when(it + 2 < CHUNKS)
                    def _():
                        prepare(t, it + 2)
                        own_copy(it + 2).start()

                @pl.when(outer)
                def _():
                    picked(it).wait_recv()

                @pl.when((t == 0) & (it == 0))
                def _():
                    for copy in loads:
                        copy.wait()

                project(it)
                across(it).start()

                @pl.when(inner)
                def _():
                    own_copy(it).wait_send()
                    relay(it).wait_send()

                @pl.when(outer)
                def _():
                    to_inner(it).wait_send()

                across(it).wait_recv()
                activate(it)
                across(it).wait_send()
                lower(it)

                @pl.when(outer)
                def _():
                    back(it).start()

            @pl.when(inner & (it >= 2) & (it < CHUNKS + 2))
            def _():
                c = it - 2
                back(c).wait_recv()

                @pl.when(c >= 2)
                def _():
                    cross_to_outer(c - 2).wait_send()
                    cross_to_inner(c - 2).wait_send()

                cross(t, c)
                cross_to_outer(c).start()
                cross_to_inner(c).start()

            @pl.when(it >= 3)
            def _():
                c = it - 3

                @pl.when(inner)
                def _():
                    @pl.when(c >= 2)
                    def _():
                        home(c - 2).wait_send()

                    cross_to_outer(c).wait_recv()
                    bring_home(t, c)
                    home(c).start()
                    cross_to_inner(c).wait_recv()

                @pl.when(outer)
                def _():
                    own_part(t, c)
                    home(c).wait_recv()

                finish(t, c)

                @pl.when((t == 0) & (section < sections - 1))
                def _():
                    to_next(c).start()

        @pl.when(inner)
        def _():
            for c in (CHUNKS - 2, CHUNKS - 1):
                picked(c).wait_send()
                cross_to_outer(c).wait_send()
                cross_to_inner(c).wait_send()
                home(c).wait_send()

        @pl.when(outer)
        def _():
            for c in range(CHUNKS):
                back(c).wait_send()

        best = peak_pair[t]
        for k in range(1, 4):
            other = lax.rem(node + k, 4)
            pltpu.make_async_remote_copy(
                src_ref=peak_pair.at[t], dst_ref=peak_far.at[t, other], send_sem=far_send.at[t, k - 1],
                recv_sem=far_recv.at[t, other], device_id=at_node(other), device_id_type=MESH_ID,
            ).wait_recv()
            best = jnp.maximum(best, peak_far[t, other])
        scale_tile[...] = best
        peak_out[t] = best
        mate_copy(t).wait_send()
        for k in range(1, 4):
            far_copy(t, k).wait_send()

    write_out(1)
    for copy in table_copies:
        copy.wait_send()

    @pl.when(section < sections - 1)
    def _():
        index_copy.wait_send()

        @pl.loop(0, CHUNKS)
        def _(c):
            to_next(c).wait_send()

    @pl.loop(0, tiles)
    def _(k):
        store_copy(0, k).wait()
        store_copy(1, k).wait()


def fused_shards(act_in, next_in, routes, route_w, hist, gate_w, up_w, down_w):
    ticks, _, tokens, top = routes.shape
    width = act_in.shape[2]
    ffw = gate_w.shape[3]
    experts = lax.axis_size("node")
    span = tokens // CHUNKS
    capacity = 5 * tokens * top // (4 * experts)
    pick = 3 * ((capacity + (experts - 1) * (CHUNKS - 1)) // CHUNKS)
    pick = -(-pick // 16) * 16
    assert pick == 2 * span and span % 16 == 0 and width % TILE == 0 and ffw % 256 == 0
    table, index = routing_rows(routes[:, 0], route_w[:, 0], experts, CHUNKS)
    f32, bf16 = jnp.float32, jnp.bfloat16
    vmem, anywhere = pl.BlockSpec(memory_space=pltpu.VMEM), pl.BlockSpec(memory_space=pl.ANY)
    dma = pltpu.SemaphoreType.DMA
    tiles = width // TILE
    out, peaks = pl.pallas_call(
        functools.partial(fused_kernel, lax.axis_size("section"), experts),
        out_shape=(
            jax.ShapeDtypeStruct((ticks, tokens, width), bf16),
            jax.ShapeDtypeStruct((ticks, 8, 128), f32),
        ),
        in_specs=[anywhere, anywhere, vmem, vmem, vmem, anywhere, anywhere, anywhere],
        out_specs=(anywhere, vmem),
        scratch_shapes=[
            pltpu.VMEM((2, tokens, width), bf16),
            pltpu.VMEM((width, ffw), bf16),
            pltpu.VMEM((width, ffw), bf16),
            pltpu.VMEM((ffw, width), bf16),
            pltpu.VMEM((CHUNKS, tokens, width), bf16),
            pltpu.VMEM((2, tokens, width), bf16),
            pltpu.VMEM((2, pick, width), bf16),
            pltpu.VMEM((2, 2 * span, width), bf16),
            pltpu.VMEM((2, span, width), bf16),
            pltpu.VMEM((CHUNKS, pick, width), bf16),
            pltpu.VMEM((2, span, width), f32),
            pltpu.VMEM((CHUNKS, span, width), bf16),
            pltpu.VMEM((CHUNKS, span, width), bf16),
            pltpu.VMEM((tokens, 2 * ffw), bf16),
            pltpu.VMEM((2, tokens, 2 * ffw), bf16),
            pltpu.VMEM((tokens, 2 * ffw), f32),
            pltpu.VMEM((tokens, ffw), bf16),
            pltpu.VMEM((tokens, tokens), bf16),
            pltpu.VMEM((experts, ticks, CHUNKS, 2 * experts, 128), f32),
            pltpu.VMEM((8, tokens), f32),
            pltpu.VMEM((8, 128), f32),
            pltpu.VMEM((ticks, 8, 128), f32),
            pltpu.VMEM((ticks, 8, 128), f32),
            pltpu.VMEM((ticks, 8, 128), f32),
            pltpu.VMEM((ticks, experts, 8, 128), f32),
            dma((KINDS, CHUNKS)),
            dma((KINDS, CHUNKS)),
            dma((5,)),
            dma((ticks, tiles)),
            dma((experts - 1,)),
            dma((experts,)),
            dma((2,)),
            dma((2, ticks)),
            dma((ticks, experts - 1)),
            dma((ticks, experts)),
        ],
        compiler_params=pltpu.CompilerParams(has_side_effects=True, vmem_limit_bytes=67043328),
        name="fused_stack",
    )(
        act_in[0], next_in, table, index, hist.reshape(1, 1), gate_w[0, 0], up_w[0, 0], down_w[0, 0]
    )
    return out[:, None], peaks[:, 0, 0][None, :]


def solution(mesh):
    fused = mesh.shape["node"] == 4 and mesh.shape["torus"] == 2
    return jax.shard_map(
        fused_shards if fused else shards,
        mesh=mesh,
        in_specs=(
            P("section", "node", "torus"),
            P("node", "torus"),
            P(None, "section", "node", None),
            P(None, "section", "node", None),
            P("section"),
            P("section", "node", "torus", None),
            P("section", "node", "torus", None),
            P("section", "node", None, "torus"),
        ),
        out_specs=(P(None, "section", "node", "torus"), P("section", None)),
        check_vma=False,
    )
```

```python
import functools

import jax
import jax.numpy as jnp
from jax import lax
from jax.experimental import pallas as pl
from jax.experimental.pallas import tpu as pltpu
from jax.sharding import PartitionSpec as P

FP8_LIMIT = 448.0
MAX_CHUNKS = 4
DEPTH = 2


def shifted(value, axis, steps):
    count = lax.axis_size(axis)
    return lax.ppermute(value, axis, [(i, (i + steps) % count) for i in range(count)])


def swapped(value, axis):
    count = lax.axis_size(axis)
    return lax.ppermute(value, axis, [(i, i ^ 1) for i in range(count)])


def to_next_section(value):
    count = lax.axis_size("section")
    return lax.ppermute(value, "section", [(i, i + 1) for i in range(count - 1)])


def dot(left, right):
    return lax.dot_general(left, right, (((1,), (0,)), ((), ())), preferred_element_type=jnp.float32)


def torus_sum(value):
    if lax.axis_size("torus") == 2:
        return value + swapped(value.astype(jnp.bfloat16), "torus").astype(jnp.float32)
    return lax.psum(value, "torus")


def after(value, *earlier):
    return lax.optimization_barrier((value, *earlier))[0]


def ring_max(value, axis):
    count = lax.axis_size(axis)
    if count & (count - 1):
        return lax.pmax(value, axis)
    step = 1
    while step < count:
        value = jnp.maximum(value, shifted(value, axis, step))
        step *= 2
    return value


def routing_tables(expert_of, weight_of, capacity, n_node, me):
    tokens = expert_of.shape[0]
    pair = jnp.stack([me, me ^ 1]).astype(jnp.float32)
    named = expert_of[:, None, :] == pair[None, :, None]
    hit = jnp.any(named, axis=2)
    wgt = jnp.sum(jnp.where(named, weight_of[:, None, :], 0.0), axis=2)
    earlier = (jnp.arange(tokens)[:, None] > jnp.arange(tokens)[None, :]).astype(jnp.bfloat16)
    slots = jnp.arange(capacity, dtype=jnp.float32)
    rank = dot(earlier, hit.astype(jnp.bfloat16))
    chosen = (rank[:, :, None] == slots) & hit[:, :, None]
    table = chosen.astype(jnp.bfloat16).reshape(tokens, 2 * capacity)
    combine = jnp.where(chosen, wgt[:, :, None], 0.0).astype(jnp.bfloat16)
    return table.T, combine.reshape(tokens, 2 * capacity)


def shards(act_in, next_in, routes, route_w, hist, gate_w, up_w, down_w):
    tokens = act_in.shape[1]
    ticks = routes.shape[0]
    top = routes.shape[3]
    n_node = lax.axis_size("node")
    groups = n_node // 2
    capacity = 5 * tokens * top // (4 * n_node)
    half = groups * capacity
    gate_mat, up_mat, down_mat = gate_w[0, 0], up_w[0, 0], down_w[0, 0]
    width = gate_mat.shape[0]
    count = max(c for c in range(1, MAX_CHUNKS + 1) if width % (128 * c) == 0)
    size = width // count
    me = lax.axis_index("node")
    section_now = lax.axis_index("section")

    own_peak = jnp.max(jnp.abs(act_in[0])).astype(jnp.float32)
    packed = jnp.concatenate(
        [routes.astype(jnp.float32).reshape(-1), route_w.reshape(-1), jnp.full((128,), own_peak)]
    )
    amount = ticks * tokens * top
    known = [packed] + [shifted(packed, "node", -2 * k) for k in range(1, groups)]
    tables = []
    for tick in range(ticks):
        pairs = []
        for info in known:
            expert_of = info[:amount].reshape(ticks, tokens, top)[tick]
            weight_of = info[amount : 2 * amount].reshape(ticks, tokens, top)[tick]
            pairs.append(routing_tables(expert_of, weight_of, capacity, n_node, me))
        tables.append(tuple(zip(*pairs)))

    cuts = [slice(c * size, (c + 1) * size) for c in range(count)]
    streams = [act_in[0][:, cut] for cut in cuts]
    scale = hist[0]
    first_peak = known[0][-1:]
    for info in known[1:]:
        first_peak = jnp.maximum(first_peak, info[-1:])
    first_peak = ring_max(first_peak, "torus")
    first_peak = jnp.maximum(first_peak, swapped(first_peak, "node"))
    outputs, peaks = [], [first_peak[0]]
    for tick in range(ticks):
        select, combine = tables[tick]
        if tick > 0:
            streams = [
                lax.optimization_barrier(
                    jnp.where(section_now == 0, next_in[:, cut], to_next_section(outputs[-1][c]))
                )
                for c, cut in enumerate(cuts)
            ]
            scale = peaks[tick - 1]
        factor = FP8_LIMIT / scale
        dequant = scale / FP8_LIMIT
        gate = up = None
        sent = []
        for c, cut in enumerate(cuts):
            quantized = jnp.clip(
                streams[c].astype(jnp.float32) * factor, -FP8_LIMIT, FP8_LIMIT
            ).astype(jnp.bfloat16)
            if c >= DEPTH:
                quantized = after(quantized, sent[c - DEPTH], first_peak)
            if tick > 0 and c == count - 1:
                seen = [after(s, sent[0]) if sent else s for s in streams]
                here = [jnp.max(jnp.abs(s)).astype(jnp.float32).reshape(1) for s in seen]
                here = jnp.max(jnp.concatenate(here), keepdims=True)
                here = ring_max(ring_max(here, "torus"), "node")
                peaks.append(here[0])
                quantized = after(quantized, here)
            elif tick == 0:
                quantized = after(quantized, known[-1])
            held = [quantized] + [shifted(quantized, "node", -2 * k) for k in range(1, groups)]
            picked = [dot(select[k], held[k]).astype(jnp.bfloat16) for k in range(groups)]
            mine = jnp.concatenate([p[:capacity] for p in picked], axis=0)
            sent.append(jnp.concatenate([p[capacity:] for p in picked], axis=0))
            rows = jnp.concatenate([mine, swapped(sent[c], "node")], axis=0)
            gate_part = dot(rows, gate_mat[cut])
            up_part = dot(rows, up_mat[cut])
            gate = gate_part if gate is None else gate + gate_part
            up = up_part if up is None else up + up_part
        gate = torus_sum(gate) * dequant
        up = torus_sum(up) * dequant
        hidden = (jax.nn.silu(gate) * up).astype(jnp.bfloat16)
        layer, crossed = [], []
        for c, cut in enumerate(cuts):
            away_rows = hidden[half:]
            if c >= DEPTH:
                away_rows = after(away_rows, crossed[c - DEPTH])
            away = dot(away_rows, down_mat[:, cut]).astype(jnp.bfloat16)
            home_rows = after(hidden[:half], away)
            home = dot(home_rows, down_mat[:, cut]).astype(jnp.bfloat16)
            back = swapped(away, "node")
            branch = None
            for k in reversed(range(groups)):
                span = slice(k * capacity, (k + 1) * capacity)
                part = dot(combine[k], jnp.concatenate([home[span], back[span]], axis=0))
                if k > 0:
                    part = part.astype(jnp.bfloat16)
                    crossed = crossed + [part] if k == groups - 1 else crossed
                    part = shifted(part, "node", 2 * k).astype(jnp.float32)
                branch = part if branch is None else branch + part
            layer.append((streams[c].astype(jnp.float32) + branch).astype(jnp.bfloat16))
        outputs.append(layer)
    act_out = jnp.stack([jnp.concatenate(layer, axis=1) for layer in outputs])
    return act_out[:, None], jnp.stack(peaks)[None, :]


MESH_ID = pl.DeviceIdType.MESH
CHUNKS = 4
OWN, TO_INNER, RELAY, PICKED, BACK, CROSS_OUT, CROSS_IN, HOME, NEXT, TORUS, KINDS = range(11)
TILE = 512
PIECES = 2
HALVES = 2


def fused_kernel(
    sections, experts, act_hbm, next_hbm, routes, route_w, hist, gate_hbm, up_hbm, down_hbm,
    out_hbm, peak_out, index,
    inputs, gate_mat, up_mat, down_mat, rows, stream, picked_out, cross_out, home_out,
    back_in, own_sum, cross_in, cross_own, torus_out, torus_in, partial, hidden, order,
    tables, index_prev, scale_tile, peak_own, peak_pair, peak_mate, peak_far,
    send, recv, load_sem, store_sem, table_send, table_recv, index_sem, mate_sem, far_send, far_recv,
):
    tokens, width = act_hbm.shape
    source, arrived = inputs.at[0], inputs.at[1]
    ffw = down_hbm.shape[0]
    span = tokens // CHUNKS
    pick = picked_out.shape[1]
    tiles = width // TILE
    halves, step = HALVES, 256
    blocks = ffw // step // halves
    section, node, torus = (lax.axis_index(a) for a in ("section", "node", "torus"))
    outer = (node == 0) | (node == 3)
    inner = jnp.logical_not(outer)
    side = node // 2
    mate = jnp.where(outer, 1 + side, 3 * side)
    facing = 2 - side
    far = 3 - 3 * side
    here_in, here_out = 1 + side, 3 * side
    f32, bf16 = jnp.float32, jnp.bfloat16

    pieces = min(PIECES, tiles)
    bounds = [-(-tiles * h // pieces) for h in range(pieces + 1)]

    def move(kind, c, src, dst, target, h=0):
        return pltpu.make_async_remote_copy(
            src_ref=src, dst_ref=dst, send_sem=send.at[kind, c, h], recv_sem=recv.at[kind, c, h],
            device_id=target, device_id_type=MESH_ID,
        )

    def cut(h):
        return slice(bounds[h] * TILE, bounds[h + 1] * TILE)

    def piece_tiles(h):
        return [slice(k * TILE, (k + 1) * TILE) for k in range(bounds[h], bounds[h + 1])]

    def at_node(n):
        return (section, n, torus)

    def part(c, first, h=None, count=1):
        return rows.at[c, pl.ds(first * span, count * span), slice(None) if h is None else cut(h)]

    def own_copy(c, h):
        return move(OWN, c, part(c, 1, h), part(c, 2, h), at_node(facing), h)

    def to_inner(c, h):
        return move(TO_INNER, c, part(c, 1, h), part(c, 0, h), at_node(mate), h)

    def relay(c, h):
        return move(RELAY, c, part(c, 0, h), part(c, 3, h), at_node(facing), h)

    def picked(c, h):
        return move(PICKED, c, picked_out.at[c % 2, :, cut(h)], part(c, 2, h, 2), at_node(mate), h)

    def back(c, h):
        return move(BACK, c, part(c, 2, h, 2), back_in.at[c, :, cut(h)], at_node(mate), h)

    def cross_to_outer(c, h):
        src = cross_out.at[c % 2, pl.ds(span, span), cut(h)]
        return move(CROSS_OUT, c, src, cross_in.at[c, :, cut(h)], at_node(facing), h)

    def cross_to_inner(c, h):
        src = cross_out.at[c % 2, pl.ds(0, span), cut(h)]
        return move(CROSS_IN, c, src, cross_own.at[c, :, cut(h)], at_node(facing), h)

    def home(c, h):
        return move(HOME, c, home_out.at[c % 2, :, cut(h)], cross_own.at[c, :, cut(h)], at_node(mate), h)

    def to_next(c, h):
        strip = pl.ds(c * span, span)
        src, dst = stream.at[0, strip, cut(h)], arrived.at[strip, cut(h)]
        return move(NEXT, c, src, dst, (section + 1, node, torus), h)

    def wait_all(end, *copies):
        for copy in copies:
            for h in range(pieces):
                getattr(copy(h), end)()

    def across(c, h):
        part_width = 2 * ffw // halves
        strip = slice(h * part_width, (h + 1) * part_width)
        return move(
            TORUS, c, torus_out.at[:, strip], torus_in.at[c % 2, :, strip], (section, node, 1 - torus), h
        )

    def eye(count):
        return lax.broadcasted_iota(jnp.int32, (count, count), 0) == lax.broadcasted_iota(
            jnp.int32, (count, count), 1
        )

    def column(row):
        count = row.shape[1]
        return jnp.sum(jnp.where(eye(count), row, 0.0), axis=1, keepdims=True)

    def row_of(block, number):
        at = lax.broadcasted_iota(jnp.int32, block.shape, 0) == number
        return jnp.sum(jnp.where(at, block, 0.0), axis=0, keepdims=True)

    def sort_tokens(t):
        picks = [routes[t, k : k + 1, :] for k in range(routes.shape[1])]
        low, high = functools.reduce(jnp.minimum, picks), functools.reduce(jnp.maximum, picks)
        lane = lax.broadcasted_iota(jnp.int32, (1, tokens), 1)
        key = ((low * experts + high) * tokens + lane).astype(f32)
        place = jnp.sum(jnp.where(column(key) < key, 1.0, 0.0), axis=0, keepdims=True).astype(jnp.int32)
        spot = (place & (CHUNKS - 1)) * span + (place >> (CHUNKS.bit_length() - 1))
        index[t] = jnp.broadcast_to(spot.astype(f32), (8, tokens))

    def make_table(t):
        at = jnp.where(column(index[t][0:1]) == places(tokens, tokens, 1), 1.0, 0.0).astype(bf16)
        lines = []
        for weighted in (True, False):
            for e in range(experts):
                line = jnp.zeros((1, tokens), f32)
                for k in range(routes.shape[1]):
                    value = route_w[t, k : k + 1, :] if weighted else 1.0
                    line = line + jnp.where(routes[t, k : k + 1, :] == e, value, 0.0)
                lines.append(line)
        rest = jnp.concatenate(lines, axis=0)
        block = jnp.zeros_like(rest)
        for _ in range(3):
            term = rest.astype(bf16)
            block = block + dot(term, at)
            rest = rest - term.astype(f32)
        keep = lax.broadcasted_iota(jnp.int32, (2 * experts, 128), 1) < span
        for c in range(CHUNKS):
            first = c * span // 128 * 128
            half = block[:, first : first + 128]
            if c * span % 128:
                half = pltpu.roll(half, 128 - c * span % 128, 1)
            tables[node, t, c] = jnp.where(keep, half, 0.0)

    def spread(t, c):
        left = tables[here_out, t, c] + pltpu.roll(tables[here_in, t, c], span, 1)
        right = tables[facing, t, c] + pltpu.roll(tables[far, t, c], span, 1)
        return jnp.concatenate([left, right], axis=1)

    def outer_ranks(block):
        count = block.shape[1]
        lanes = lax.broadcasted_iota(jnp.int32, (1, count), 1)
        hit = jnp.where(lanes >= span, row_of(block, experts + here_out), 0.0)
        before = lax.broadcasted_iota(jnp.int32, (count, count), 0) < lax.broadcasted_iota(
            jnp.int32, (count, count), 1
        )
        wide = jnp.broadcast_to(hit, (8, count)).astype(bf16)
        rank = dot(wide, jnp.where(before, 1.0, 0.0).astype(bf16))[0:1]
        return jnp.where(hit > 0.0, rank, -1.0)

    def places(count, other, axis):
        return lax.broadcasted_iota(jnp.int32, (count, other), axis).astype(f32)

    def tile_at(k):
        return pl.ds(pl.multiple_of(k * TILE, TILE), TILE)

    def prepare(t, c, h):
        factor = FP8_LIMIT / scale_tile[0:1, 0:1]
        strip = pl.ds(pl.multiple_of(c * span, span), span)
        for cols in piece_tiles(h):
            value = dot(order[strip, :], inputs[t, :, cols])
            stream[t, strip, cols] = value.astype(bf16)
            top = jnp.max(jnp.max(jnp.abs(value), axis=0, keepdims=True), axis=1, keepdims=True)
            peak_own[t] = jnp.maximum(peak_own[t], top)
            rows[c, pl.ds(span, span), cols] = jnp.clip(
                value * factor, -FP8_LIMIT, FP8_LIMIT
            ).astype(bf16)

    def select_for_outer(t, c):
        rank = outer_ranks(spread(t, c))
        table_mat = jnp.where(places(pick, tokens, 0) == rank, 1.0, 0.0).astype(bf16)

        for h in range(pieces):
            @pl.loop(bounds[h], bounds[h + 1])
            def _(k):
                cols = tile_at(k)
                picked_out[c % 2, :, cols] = dot(table_mat, rows[c, :, cols]).astype(bf16)

            picked(c, h).start()

    def project(c):
        for h in range(halves):
            @pl.loop(h * blocks, (h + 1) * blocks)
            def _(k):
                cols = pl.ds(pl.multiple_of(k * step, step), step)
                for turn, mat in enumerate((gate_mat, up_mat)):
                    place = pl.ds(pl.multiple_of((2 * k + turn) * step, step), step)
                    value = dot(rows[c], mat[:, cols])
                    partial[:, place] = value
                    torus_out[:, place] = value.astype(bf16)

            across(c, h).start()

    def activate(c):
        dequant = scale_tile[0:1, 0:1] / FP8_LIMIT
        for h in range(halves):
            across(c, h).wait_recv()

            @pl.loop(h * blocks, (h + 1) * blocks)
            def _(k):
                both = []
                for turn in range(2):
                    place = pl.ds(pl.multiple_of((2 * k + turn) * step, step), step)
                    both.append((partial[:, place] + torus_in[c % 2, :, place].astype(f32)) * dequant)
                gate, up = both
                cols = pl.ds(pl.multiple_of(k * step, step), step)
                hidden[:, cols] = (gate / (1.0 + jnp.exp(-gate)) * up).astype(bf16)

        for h in range(halves):
            across(c, h).wait_send()

    def lower(c):
        for h in range(pieces):
            @pl.loop(bounds[h], bounds[h + 1])
            def _(k):
                cols = tile_at(k)
                rows[c, :, cols] = dot(hidden[...], down_mat[:, cols]).astype(bf16)

            @pl.when(outer)
            def _():
                back(c, h).start()

    def cross(t, c):
        block = spread(t, c)
        rank = column(outer_ranks(block))[span:]
        scatter = jnp.where(places(tokens - span, pick, 1) == rank, 1.0, 0.0).astype(bf16)
        weight_in = column(row_of(block, here_in))[span:]
        weight_out = column(row_of(block, here_out))[span:]
        for h in range(pieces):
            back(c, h).wait_recv()
            for cols in piece_tiles(h):
                value = weight_out * dot(scatter, back_in[c, :, cols])
                value = value + weight_in * rows[c, pl.ds(span, tokens - span), cols].astype(f32)
                own_sum[c % 2, :, cols] = value[:span]
                cross_out[c % 2, :, cols] = value[span:].astype(bf16)
            cross_to_outer(c, h).start()
            cross_to_inner(c, h).start()

    def bring_home(t, c, h):
        weight = column(row_of(tables[here_out, t, c], here_in))[:span]
        for cols in piece_tiles(h):
            value = weight * rows[c, pl.ds(0, span), cols].astype(f32) + cross_in[c, :, cols].astype(f32)
            home_out[c % 2, :, cols] = value.astype(bf16)

    def own_part(t, c):
        weight = column(row_of(tables[node, t, c], node))[:span]

        @pl.loop(0, tiles)
        def _(k):
            cols = tile_at(k)
            own_sum[c % 2, :, cols] = weight * rows[c, pl.ds(span, span), cols].astype(f32)

    def finish(t, c, h):
        strip = pl.ds(pl.multiple_of(c * span, span), span)
        for cols in piece_tiles(h):
            value = stream[t, strip, cols].astype(f32) + own_sum[c % 2, :, cols]
            stream[t, strip, cols] = (value + cross_own[c, :, cols].astype(f32)).astype(bf16)

    def store_copy(t, c, h):
        strip = pl.ds(pl.multiple_of(c * span, span), span)
        return pltpu.make_async_copy(
            stream.at[t, strip, cut(h)], out_hbm.at[t, strip, cut(h)], store_sem.at[t, c, h]
        )

    first_load = pltpu.make_async_copy(act_hbm, source, load_sem.at[0])
    first_load.start()
    next_load = pltpu.make_async_copy(next_hbm, arrived, load_sem.at[1])
    loads = [
        pltpu.make_async_copy(hbm, mat, load_sem.at[2 + i])
        for i, (hbm, mat) in enumerate(((gate_hbm, gate_mat), (up_hbm, up_mat), (down_hbm, down_mat)))
    ]
    table_copies = []
    for k in range(1, 4):
        other = lax.rem(node + k, 4)
        table_copies.append(
            pltpu.make_async_remote_copy(
                src_ref=tables.at[node], dst_ref=tables.at[node], send_sem=table_send.at[k - 1],
                recv_sem=table_recv.at[node], device_id=at_node(other), device_id_type=MESH_ID,
            )
        )
    index_copy = pltpu.make_async_remote_copy(
        src_ref=index.at[0], dst_ref=index_prev, send_sem=index_sem.at[0], recv_sem=index_sem.at[1],
        device_id=(section + 1, node, torus), device_id_type=MESH_ID,
    )

    def mate_copy(t):
        return pltpu.make_async_remote_copy(
            src_ref=peak_own.at[t], dst_ref=peak_mate.at[t], send_sem=mate_sem.at[0, t],
            recv_sem=mate_sem.at[1, t], device_id=(section, node, 1 - torus), device_id_type=MESH_ID,
        )

    def far_copy(t, k):
        return pltpu.make_async_remote_copy(
            src_ref=peak_pair.at[t], dst_ref=peak_far.at[t, node], send_sem=far_send.at[t, k - 1],
            recv_sem=far_recv.at[t, node], device_id=at_node(lax.rem(node + k, 4)), device_id_type=MESH_ID,
        )

    scale_tile[...] = jnp.broadcast_to(hist[...], scale_tile.shape)
    peak_own[...] = jnp.zeros_like(peak_own)
    for copy in loads:
        copy.start()
    sort_tokens(0)
    order[...] = jnp.where(places(tokens, tokens, 0) == index[0][0:1], 1.0, 0.0).astype(bf16)

    @pl.when(section < sections - 1)
    def _():
        index_copy.start()

    @pl.when(section == 0)
    def _():
        next_load.start()
        index_prev[...] = places(8, tokens, 1)

    first_load.wait()

    @pl.loop(0, 2)
    def _(t):
        @pl.when(t == 1)
        def _():
            @pl.when(section == 0)
            def _():
                next_load.wait()

        for h in range(pieces):
            @pl.when((t == 1) & (section > 0))
            def _():
                for c in range(CHUNKS):
                    to_next(c, h).wait_recv()

            prepare(t, 0, h)

            @pl.when(outer)
            def _():
                to_inner(0, h).start()

            @pl.when(inner)
            def _():
                own_copy(0, h).start()

            if h == 0:
                @pl.when(t == 0)
                def _():
                    sort_tokens(1)
                    make_table(0)
                    make_table(1)
                    for copy in table_copies:
                        copy.start()

            @pl.when(inner)
            def _():
                to_inner(0, h).wait_recv()
                relay(0, h).start()

        @pl.loop(1, jnp.where(outer, CHUNKS, 2))
        def _(c):
            for h in range(pieces):
                prepare(t, c, h)

                @pl.when(outer)
                def _():
                    to_inner(c, h).start()

                @pl.when(inner)
                def _():
                    own_copy(c, h).start()

        @pl.when(t == 0)
        def _():
            @pl.when(outer)
            def _():
                rows[:, 0:span, :] = jnp.zeros((CHUNKS, span, width), bf16)

            for k in range(1, 4):
                other = lax.rem(node + k, 4)
                pltpu.make_async_remote_copy(
                    src_ref=tables.at[node], dst_ref=tables.at[other], send_sem=table_send.at[k - 1],
                    recv_sem=table_recv.at[other], device_id=at_node(other), device_id_type=MESH_ID,
                ).wait_recv()

        @pl.loop(0, CHUNKS + 3)
        def _(it):
            @pl.when(it == 2)
            def _():
                mate_copy(t).start()

            @pl.when(it == 3)
            def _():
                mate_copy(t).wait_recv()
                peak_pair[t] = jnp.maximum(peak_own[t], peak_mate[t])
                for k in range(1, 4):
                    far_copy(t, k).start()

            @pl.when(it < CHUNKS)
            def _():
                @pl.when(inner)
                def _():
                    wait_all("wait_recv", lambda h: own_copy(it, h), lambda h: relay(it, h))

                    @pl.when((t > 0) | (it >= 2))
                    def _():
                        wait_all("wait_send", lambda h: picked(lax.rem(it + 2, CHUNKS), h))

                    select_for_outer(t, it)

                    @pl.when(it + 1 < CHUNKS)
                    def _():
                        for h in range(pieces):
                            to_inner(it + 1, h).wait_recv()
                            relay(it + 1, h).start()

                    @pl.when(it + 2 < CHUNKS)
                    def _():
                        for h in range(pieces):
                            prepare(t, it + 2, h)
                            own_copy(it + 2, h).start()

                @pl.when(outer)
                def _():
                    wait_all("wait_recv", lambda h: picked(it, h))

                @pl.when((t == 0) & (it == 0))
                def _():
                    for copy in loads:
                        copy.wait()

                project(it)

                @pl.when(inner)
                def _():
                    wait_all("wait_send", lambda h: own_copy(it, h), lambda h: relay(it, h))

                @pl.when(outer)
                def _():
                    wait_all("wait_send", lambda h: to_inner(it, h))

                activate(it)
                lower(it)

            @pl.when(inner & (it >= 2) & (it < CHUNKS + 2))
            def _():
                c = it - 2
                @pl.when((t > 0) | (c >= 2))
                def _():
                    last = lax.rem(c + 2, CHUNKS)
                    wait_all("wait_send", lambda h: cross_to_outer(last, h), lambda h: cross_to_inner(last, h))

                cross(t, c)

            @pl.when(it == CHUNKS + 2)
            def _():
                best = peak_pair[t]
                for k in range(1, 4):
                    other = lax.rem(node + k, 4)
                    pltpu.make_async_remote_copy(
                        src_ref=peak_pair.at[t], dst_ref=peak_far.at[t, other], send_sem=far_send.at[t, k - 1],
                        recv_sem=far_recv.at[t, other], device_id=at_node(other), device_id_type=MESH_ID,
                    ).wait_recv()
                    best = jnp.maximum(best, peak_far[t, other])
                scale_tile[...] = best
                peak_out[t] = best
                mate_copy(t).wait_send()
                for k in range(1, 4):
                    far_copy(t, k).wait_send()

                @pl.when(t == 0)
                def _():
                    @pl.when(section > 0)
                    def _():
                        index_copy.wait_recv()

                    now = jnp.where(places(tokens, tokens, 0) == index[1][0:1], 1.0, 0.0).astype(bf16)
                    was = jnp.where(places(tokens, tokens, 0) == index_prev[0:1], 1.0, 0.0).astype(bf16)
                    order[...] = lax.dot_general(
                        now, was, (((1,), (1,)), ((), ())), preferred_element_type=f32
                    ).astype(bf16)

            @pl.when(it >= 3)
            def _():
                c = it - 3

                @pl.when(inner & ((t > 0) | (c >= 2)))
                def _():
                    wait_all("wait_send", lambda h: home(lax.rem(c + 2, CHUNKS), h))

                @pl.when(outer)
                def _():
                    own_part(t, c)

                for h in range(pieces):
                    @pl.when(inner)
                    def _():
                        cross_to_outer(c, h).wait_recv()
                        bring_home(t, c, h)
                        home(c, h).start()
                        cross_to_inner(c, h).wait_recv()

                    @pl.when(outer)
                    def _():
                        home(c, h).wait_recv()

                    finish(t, c, h)

                    @pl.when((t == 0) & (section < sections - 1))
                    def _():
                        to_next(c, h).start()

                    store_copy(t, c, h).start()

        @pl.when(outer)
        def _():
            for c in range(CHUNKS):
                wait_all("wait_send", lambda h: back(c, h))

    @pl.when(inner)
    def _():
        for c in (CHUNKS - 2, CHUNKS - 1):
            wait_all(
                "wait_send", lambda h: picked(c, h), lambda h: cross_to_outer(c, h),
                lambda h: cross_to_inner(c, h), lambda h: home(c, h),
            )

    for copy in table_copies:
        copy.wait_send()

    @pl.when(section < sections - 1)
    def _():
        index_copy.wait_send()

        @pl.loop(0, CHUNKS)
        def _(c):
            wait_all("wait_send", lambda h: to_next(c, h))

    @pl.loop(0, CHUNKS)
    def _(c):
        wait_all("wait", lambda h: store_copy(0, c, h), lambda h: store_copy(1, c, h))


def restore_kernel(dealt, peaks, index, out, peak_out):
    tokens = index.shape[2]
    ticks = peak_out.shape[1]
    down = lax.broadcasted_iota(jnp.int32, (tokens, tokens), 0)
    along = lax.broadcasted_iota(jnp.int32, (tokens, tokens), 1)
    spot = jnp.sum(jnp.where(down == along, index[0, 0:1, :], 0.0), axis=1, keepdims=True)
    undo = jnp.where(along.astype(jnp.float32) == spot, 1.0, 0.0).astype(jnp.bfloat16)
    out[0] = dot(undo, dealt[0]).astype(jnp.bfloat16)
    lane = lax.broadcasted_iota(jnp.int32, (1, ticks), 1)
    line = jnp.zeros((1, ticks), jnp.float32)
    for t in range(ticks):
        line = jnp.where(lane == t, peaks[t, 0:1, 0:1], line)
    peak_out[...] = line


def fused_shards(act_in, next_in, routes, route_w, hist, gate_w, up_w, down_w):
    ticks, _, tokens, top = routes.shape
    width = act_in.shape[2]
    ffw = gate_w.shape[3]
    experts = lax.axis_size("node")
    span = tokens // CHUNKS
    capacity = 5 * tokens * top // (4 * experts)
    pick = 3 * ((capacity + (experts - 1) * (CHUNKS - 1)) // CHUNKS)
    pick = -(-pick // 16) * 16
    assert pick == 2 * span and span % 16 == 0 and width % TILE == 0 and ffw % 256 == 0
    by_rank = lambda value: value[:, 0].transpose(0, 2, 1)
    f32, bf16 = jnp.float32, jnp.bfloat16
    vmem, anywhere = pl.BlockSpec(memory_space=pltpu.VMEM), pl.BlockSpec(memory_space=pl.ANY)
    dma = pltpu.SemaphoreType.DMA
    tiles = width // TILE
    out, peaks, index = pl.pallas_call(
        functools.partial(fused_kernel, lax.axis_size("section"), experts),
        out_shape=(
            jax.ShapeDtypeStruct((ticks, tokens, width), bf16),
            jax.ShapeDtypeStruct((ticks, 8, 128), f32),
            jax.ShapeDtypeStruct((ticks, 8, tokens), f32),
        ),
        in_specs=[anywhere, anywhere, vmem, vmem, vmem, anywhere, anywhere, anywhere],
        out_specs=(anywhere, vmem, vmem),
        scratch_shapes=[
            pltpu.VMEM((2, tokens, width), bf16),
            pltpu.VMEM((width, ffw), bf16),
            pltpu.VMEM((width, ffw), bf16),
            pltpu.VMEM((ffw, width), bf16),
            pltpu.VMEM((CHUNKS, tokens, width), bf16),
            pltpu.VMEM((2, tokens, width), bf16),
            pltpu.VMEM((2, pick, width), bf16),
            pltpu.VMEM((2, 2 * span, width), bf16),
            pltpu.VMEM((2, span, width), bf16),
            pltpu.VMEM((CHUNKS, pick, width), bf16),
            pltpu.VMEM((2, span, width), f32),
            pltpu.VMEM((CHUNKS, span, width), bf16),
            pltpu.VMEM((CHUNKS, span, width), bf16),
            pltpu.VMEM((tokens, 2 * ffw), bf16),
            pltpu.VMEM((2, tokens, 2 * ffw), bf16),
            pltpu.VMEM((tokens, 2 * ffw), f32),
            pltpu.VMEM((tokens, ffw), bf16),
            pltpu.VMEM((tokens, tokens), bf16),
            pltpu.VMEM((experts, ticks, CHUNKS, 2 * experts, 128), f32),
            pltpu.VMEM((8, tokens), f32),
            pltpu.VMEM((8, 128), f32),
            pltpu.VMEM((ticks, 8, 128), f32),
            pltpu.VMEM((ticks, 8, 128), f32),
            pltpu.VMEM((ticks, 8, 128), f32),
            pltpu.VMEM((ticks, experts, 8, 128), f32),
            dma((KINDS, CHUNKS, PIECES)),
            dma((KINDS, CHUNKS, PIECES)),
            dma((5,)),
            dma((ticks, CHUNKS, PIECES)),
            dma((experts - 1,)),
            dma((experts,)),
            dma((2,)),
            dma((2, ticks)),
            dma((ticks, experts - 1)),
            dma((ticks, experts)),
        ],
        compiler_params=pltpu.CompilerParams(has_side_effects=True, vmem_limit_bytes=67043328),
        name="fused_stack",
    )(
        act_in[0], next_in, by_rank(routes), by_rank(route_w), hist.reshape(1, 1), gate_w[0, 0], up_w[0, 0], down_w[0, 0]
    )
    block = width // 2
    out, peaks = pl.pallas_call(
        restore_kernel,
        grid=(ticks, width // block),
        out_shape=(
            jax.ShapeDtypeStruct((ticks, tokens, width), bf16),
            jax.ShapeDtypeStruct((1, ticks), f32),
        ),
        in_specs=[
            pl.BlockSpec((1, tokens, block), lambda t, k: (t, 0, k)),
            pl.BlockSpec((ticks, 8, 128), lambda t, k: (0, 0, 0)),
            pl.BlockSpec((1, 8, tokens), lambda t, k: (t, 0, 0)),
        ],
        out_specs=(
            pl.BlockSpec((1, tokens, block), lambda t, k: (t, 0, k)),
            pl.BlockSpec((1, ticks), lambda t, k: (0, 0)),
        ),
        name="restore_order",
    )(out, peaks, index)
    return out[:, None], peaks


def solution(mesh):
    fused = mesh.shape["node"] == 4 and mesh.shape["torus"] == 2
    return jax.shard_map(
        fused_shards if fused else shards,
        mesh=mesh,
        in_specs=(
            P("section", "node", "torus"),
            P("node", "torus"),
            P(None, "section", "node", None),
            P(None, "section", "node", None),
            P("section"),
            P("section", "node", "torus", None),
            P("section", "node", "torus", None),
            P("section", "node", None, "torus"),
        ),
        out_specs=(P(None, "section", "node", "torus"), P("section", None)),
        check_vma=False,
    )
```

```python
import functools

import jax
import jax.numpy as jnp
from jax import lax
from jax.experimental import pallas as pl
from jax.experimental.pallas import tpu as pltpu
from jax.sharding import PartitionSpec as P

FP8_LIMIT = 448.0
MAX_CHUNKS = 4
DEPTH = 2


def shifted(value, axis, steps):
    count = lax.axis_size(axis)
    return lax.ppermute(value, axis, [(i, (i + steps) % count) for i in range(count)])


def swapped(value, axis):
    count = lax.axis_size(axis)
    return lax.ppermute(value, axis, [(i, i ^ 1) for i in range(count)])


def to_next_section(value):
    count = lax.axis_size("section")
    return lax.ppermute(value, "section", [(i, i + 1) for i in range(count - 1)])


def dot(left, right):
    return lax.dot_general(left, right, (((1,), (0,)), ((), ())), preferred_element_type=jnp.float32)


def torus_sum(value):
    if lax.axis_size("torus") == 2:
        return value + swapped(value.astype(jnp.bfloat16), "torus").astype(jnp.float32)
    return lax.psum(value, "torus")


def after(value, *earlier):
    return lax.optimization_barrier((value, *earlier))[0]


def ring_max(value, axis):
    count = lax.axis_size(axis)
    if count & (count - 1):
        return lax.pmax(value, axis)
    step = 1
    while step < count:
        value = jnp.maximum(value, shifted(value, axis, step))
        step *= 2
    return value


def routing_tables(expert_of, weight_of, capacity, n_node, me):
    tokens = expert_of.shape[0]
    pair = jnp.stack([me, me ^ 1]).astype(jnp.float32)
    named = expert_of[:, None, :] == pair[None, :, None]
    hit = jnp.any(named, axis=2)
    wgt = jnp.sum(jnp.where(named, weight_of[:, None, :], 0.0), axis=2)
    earlier = (jnp.arange(tokens)[:, None] > jnp.arange(tokens)[None, :]).astype(jnp.bfloat16)
    slots = jnp.arange(capacity, dtype=jnp.float32)
    rank = dot(earlier, hit.astype(jnp.bfloat16))
    chosen = (rank[:, :, None] == slots) & hit[:, :, None]
    table = chosen.astype(jnp.bfloat16).reshape(tokens, 2 * capacity)
    combine = jnp.where(chosen, wgt[:, :, None], 0.0).astype(jnp.bfloat16)
    return table.T, combine.reshape(tokens, 2 * capacity)


def shards(act_in, next_in, routes, route_w, hist, gate_w, up_w, down_w):
    tokens = act_in.shape[1]
    ticks = routes.shape[0]
    top = routes.shape[3]
    n_node = lax.axis_size("node")
    groups = n_node // 2
    capacity = 5 * tokens * top // (4 * n_node)
    half = groups * capacity
    gate_mat, up_mat, down_mat = gate_w[0, 0], up_w[0, 0], down_w[0, 0]
    width = gate_mat.shape[0]
    count = max(c for c in range(1, MAX_CHUNKS + 1) if width % (128 * c) == 0)
    size = width // count
    me = lax.axis_index("node")
    section_now = lax.axis_index("section")

    own_peak = jnp.max(jnp.abs(act_in[0])).astype(jnp.float32)
    packed = jnp.concatenate(
        [routes.astype(jnp.float32).reshape(-1), route_w.reshape(-1), jnp.full((128,), own_peak)]
    )
    amount = ticks * tokens * top
    known = [packed] + [shifted(packed, "node", -2 * k) for k in range(1, groups)]
    tables = []
    for tick in range(ticks):
        pairs = []
        for info in known:
            expert_of = info[:amount].reshape(ticks, tokens, top)[tick]
            weight_of = info[amount : 2 * amount].reshape(ticks, tokens, top)[tick]
            pairs.append(routing_tables(expert_of, weight_of, capacity, n_node, me))
        tables.append(tuple(zip(*pairs)))

    cuts = [slice(c * size, (c + 1) * size) for c in range(count)]
    streams = [act_in[0][:, cut] for cut in cuts]
    scale = hist[0]
    first_peak = known[0][-1:]
    for info in known[1:]:
        first_peak = jnp.maximum(first_peak, info[-1:])
    first_peak = ring_max(first_peak, "torus")
    first_peak = jnp.maximum(first_peak, swapped(first_peak, "node"))
    outputs, peaks = [], [first_peak[0]]
    for tick in range(ticks):
        select, combine = tables[tick]
        if tick > 0:
            streams = [
                lax.optimization_barrier(
                    jnp.where(section_now == 0, next_in[:, cut], to_next_section(outputs[-1][c]))
                )
                for c, cut in enumerate(cuts)
            ]
            scale = peaks[tick - 1]
        factor = FP8_LIMIT / scale
        dequant = scale / FP8_LIMIT
        gate = up = None
        sent = []
        for c, cut in enumerate(cuts):
            quantized = jnp.clip(
                streams[c].astype(jnp.float32) * factor, -FP8_LIMIT, FP8_LIMIT
            ).astype(jnp.bfloat16)
            if c >= DEPTH:
                quantized = after(quantized, sent[c - DEPTH], first_peak)
            if tick > 0 and c == count - 1:
                seen = [after(s, sent[0]) if sent else s for s in streams]
                here = [jnp.max(jnp.abs(s)).astype(jnp.float32).reshape(1) for s in seen]
                here = jnp.max(jnp.concatenate(here), keepdims=True)
                here = ring_max(ring_max(here, "torus"), "node")
                peaks.append(here[0])
                quantized = after(quantized, here)
            elif tick == 0:
                quantized = after(quantized, known[-1])
            held = [quantized] + [shifted(quantized, "node", -2 * k) for k in range(1, groups)]
            picked = [dot(select[k], held[k]).astype(jnp.bfloat16) for k in range(groups)]
            mine = jnp.concatenate([p[:capacity] for p in picked], axis=0)
            sent.append(jnp.concatenate([p[capacity:] for p in picked], axis=0))
            rows = jnp.concatenate([mine, swapped(sent[c], "node")], axis=0)
            gate_part = dot(rows, gate_mat[cut])
            up_part = dot(rows, up_mat[cut])
            gate = gate_part if gate is None else gate + gate_part
            up = up_part if up is None else up + up_part
        gate = torus_sum(gate) * dequant
        up = torus_sum(up) * dequant
        hidden = (jax.nn.silu(gate) * up).astype(jnp.bfloat16)
        layer, crossed = [], []
        for c, cut in enumerate(cuts):
            away_rows = hidden[half:]
            if c >= DEPTH:
                away_rows = after(away_rows, crossed[c - DEPTH])
            away = dot(away_rows, down_mat[:, cut]).astype(jnp.bfloat16)
            home_rows = after(hidden[:half], away)
            home = dot(home_rows, down_mat[:, cut]).astype(jnp.bfloat16)
            back = swapped(away, "node")
            branch = None
            for k in reversed(range(groups)):
                span = slice(k * capacity, (k + 1) * capacity)
                part = dot(combine[k], jnp.concatenate([home[span], back[span]], axis=0))
                if k > 0:
                    part = part.astype(jnp.bfloat16)
                    crossed = crossed + [part] if k == groups - 1 else crossed
                    part = shifted(part, "node", 2 * k).astype(jnp.float32)
                branch = part if branch is None else branch + part
            layer.append((streams[c].astype(jnp.float32) + branch).astype(jnp.bfloat16))
        outputs.append(layer)
    act_out = jnp.stack([jnp.concatenate(layer, axis=1) for layer in outputs])
    return act_out[:, None], jnp.stack(peaks)[None, :]


MESH_ID = pl.DeviceIdType.MESH
CHUNKS = 4
OWN, TO_INNER, RELAY, PICKED, BACK, CROSS_OUT, CROSS_IN, HOME, NEXT, TORUS, KINDS = range(11)
TILE = 512
PIECES = 2
HALVES = 2


def fused_kernel(
    sections, experts, act_hbm, next_hbm, routes, route_w, hist, gate_hbm, up_hbm, down_hbm,
    out_hbm, peak_out, undo,
    inputs, gate_mat, up_mat, down_mat, rows, stream, picked_out, cross_out, home_out,
    back_in, own_sum, cross_in, cross_own, torus_out, torus_in, partial, hidden, order,
    index, tables, index_prev, scale_tile, peak_own, peak_pair, peak_mate, peak_far,
    send, recv, load_sem, store_sem, table_send, table_recv, index_sem, mate_sem, far_send, far_recv,
):
    tokens, width = act_hbm.shape
    source, arrived = inputs.at[0], inputs.at[1]
    ffw = down_hbm.shape[0]
    span = tokens // CHUNKS
    pick = picked_out.shape[1]
    tiles = width // TILE
    halves, step = HALVES, 256
    blocks = ffw // step // halves
    section, node, torus = (lax.axis_index(a) for a in ("section", "node", "torus"))
    outer = (node == 0) | (node == 3)
    inner = jnp.logical_not(outer)
    side = node // 2
    mate = jnp.where(outer, 1 + side, 3 * side)
    facing = 2 - side
    far = 3 - 3 * side
    here_in, here_out = 1 + side, 3 * side
    f32, bf16 = jnp.float32, jnp.bfloat16

    pieces = min(PIECES, tiles)
    bounds = [-(-tiles * h // pieces) for h in range(pieces + 1)]

    def move(kind, c, src, dst, target, h=0):
        return pltpu.make_async_remote_copy(
            src_ref=src, dst_ref=dst, send_sem=send.at[kind, c, h], recv_sem=recv.at[kind, c, h],
            device_id=target, device_id_type=MESH_ID,
        )

    def cut(h):
        return slice(bounds[h] * TILE, bounds[h + 1] * TILE)

    def piece_tiles(h):
        return [slice(k * TILE, (k + 1) * TILE) for k in range(bounds[h], bounds[h + 1])]

    def at_node(n):
        return (section, n, torus)

    def part(c, first, h=None, count=1):
        return rows.at[c, pl.ds(first * span, count * span), slice(None) if h is None else cut(h)]

    def own_copy(c, h):
        return move(OWN, c, part(c, 1, h), part(c, 2, h), at_node(facing), h)

    def to_inner(c, h):
        return move(TO_INNER, c, part(c, 1, h), part(c, 0, h), at_node(mate), h)

    def relay(c, h):
        return move(RELAY, c, part(c, 0, h), part(c, 3, h), at_node(facing), h)

    def picked(c, h):
        return move(PICKED, c, picked_out.at[c % 2, :, cut(h)], part(c, 2, h, 2), at_node(mate), h)

    def back(c, h):
        return move(BACK, c, part(c, 2, h, 2), back_in.at[c, :, cut(h)], at_node(mate), h)

    def cross_to_outer(c, h):
        src = cross_out.at[c % 2, pl.ds(span, span), cut(h)]
        return move(CROSS_OUT, c, src, cross_in.at[c, :, cut(h)], at_node(facing), h)

    def cross_to_inner(c, h):
        src = cross_out.at[c % 2, pl.ds(0, span), cut(h)]
        return move(CROSS_IN, c, src, cross_own.at[c, :, cut(h)], at_node(facing), h)

    def home(c, h):
        return move(HOME, c, home_out.at[c % 2, :, cut(h)], cross_own.at[c, :, cut(h)], at_node(mate), h)

    def to_next(c, h):
        strip = pl.ds(c * span, span)
        src, dst = stream.at[0, strip, cut(h)], arrived.at[strip, cut(h)]
        return move(NEXT, c, src, dst, (section + 1, node, torus), h)

    def wait_all(end, *copies):
        for copy in copies:
            for h in range(pieces):
                getattr(copy(h), end)()

    def across(c, h):
        part_width = 2 * ffw // halves
        strip = slice(h * part_width, (h + 1) * part_width)
        return move(
            TORUS, c, torus_out.at[:, strip], torus_in.at[c % 2, :, strip], (section, node, 1 - torus), h
        )

    def eye(count):
        return lax.broadcasted_iota(jnp.int32, (count, count), 0) == lax.broadcasted_iota(
            jnp.int32, (count, count), 1
        )

    def column(row):
        count = row.shape[1]
        return jnp.sum(jnp.where(eye(count), row, 0.0), axis=1, keepdims=True)

    def row_of(block, number):
        at = lax.broadcasted_iota(jnp.int32, block.shape, 0) == number
        return jnp.sum(jnp.where(at, block, 0.0), axis=0, keepdims=True)

    def sort_tokens(t):
        picks = [routes[t, k : k + 1, :] for k in range(routes.shape[1])]
        low, high = functools.reduce(jnp.minimum, picks), functools.reduce(jnp.maximum, picks)
        lane = lax.broadcasted_iota(jnp.int32, (1, tokens), 1)
        key = ((low * experts + high) * tokens + lane).astype(f32)
        place = jnp.sum(jnp.where(column(key) < key, 1.0, 0.0), axis=0, keepdims=True).astype(jnp.int32)
        spot = (place & (CHUNKS - 1)) * span + (place >> (CHUNKS.bit_length() - 1))
        index[t] = jnp.broadcast_to(spot.astype(f32), (8, tokens))

    def make_table(t):
        at = jnp.where(column(index[t][0:1]) == places(tokens, tokens, 1), 1.0, 0.0).astype(bf16)
        undo[t] = at
        lines = []
        for weighted in (True, False):
            for e in range(experts):
                line = jnp.zeros((1, tokens), f32)
                for k in range(routes.shape[1]):
                    value = route_w[t, k : k + 1, :] if weighted else 1.0
                    line = line + jnp.where(routes[t, k : k + 1, :] == e, value, 0.0)
                lines.append(line)
        rest = jnp.concatenate(lines, axis=0)
        block = jnp.zeros_like(rest)
        for _ in range(3):
            term = rest.astype(bf16)
            block = block + dot(term, at)
            rest = rest - term.astype(f32)
        keep = lax.broadcasted_iota(jnp.int32, (2 * experts, 128), 1) < span
        for c in range(CHUNKS):
            first = c * span // 128 * 128
            half = block[:, first : first + 128]
            if c * span % 128:
                half = pltpu.roll(half, 128 - c * span % 128, 1)
            tables[node, t, c] = jnp.where(keep, half, 0.0)

    def spread(t, c):
        left = tables[here_out, t, c] + pltpu.roll(tables[here_in, t, c], span, 1)
        right = tables[facing, t, c] + pltpu.roll(tables[far, t, c], span, 1)
        return jnp.concatenate([left, right], axis=1)

    def outer_ranks(block):
        count = block.shape[1]
        lanes = lax.broadcasted_iota(jnp.int32, (1, count), 1)
        hit = jnp.where(lanes >= span, row_of(block, experts + here_out), 0.0)
        before = lax.broadcasted_iota(jnp.int32, (count, count), 0) < lax.broadcasted_iota(
            jnp.int32, (count, count), 1
        )
        wide = jnp.broadcast_to(hit, (8, count)).astype(bf16)
        rank = dot(wide, jnp.where(before, 1.0, 0.0).astype(bf16))[0:1]
        return jnp.where(hit > 0.0, rank, -1.0)

    def places(count, other, axis):
        return lax.broadcasted_iota(jnp.int32, (count, other), axis).astype(f32)

    def tile_at(k):
        return pl.ds(pl.multiple_of(k * TILE, TILE), TILE)

    def prepare(t, c, h):
        factor = FP8_LIMIT / scale_tile[0:1, 0:1]
        strip = pl.ds(pl.multiple_of(c * span, span), span)
        for cols in piece_tiles(h):
            value = dot(order[strip, :], inputs[t, :, cols])
            stream[t, strip, cols] = value.astype(bf16)
            top = jnp.max(jnp.max(jnp.abs(value), axis=0, keepdims=True), axis=1, keepdims=True)
            peak_own[t] = jnp.maximum(peak_own[t], top)
            rows[c, pl.ds(span, span), cols] = jnp.clip(
                value * factor, -FP8_LIMIT, FP8_LIMIT
            ).astype(bf16)

    def select_for_outer(t, c):
        rank = outer_ranks(spread(t, c))
        table_mat = jnp.where(places(pick, tokens, 0) == rank, 1.0, 0.0).astype(bf16)

        for h in range(pieces):
            @pl.loop(bounds[h], bounds[h + 1])
            def _(k):
                cols = tile_at(k)
                picked_out[c % 2, :, cols] = dot(table_mat, rows[c, :, cols]).astype(bf16)

            picked(c, h).start()

    def project(c):
        for h in range(halves):
            @pl.loop(h * blocks, (h + 1) * blocks)
            def _(k):
                cols = pl.ds(pl.multiple_of(k * step, step), step)
                for turn, mat in enumerate((gate_mat, up_mat)):
                    place = pl.ds(pl.multiple_of((2 * k + turn) * step, step), step)
                    value = dot(rows[c], mat[:, cols])
                    partial[:, place] = value
                    torus_out[:, place] = value.astype(bf16)

            across(c, h).start()

    def activate(c):
        dequant = scale_tile[0:1, 0:1] / FP8_LIMIT
        for h in range(halves):
            across(c, h).wait_recv()

            @pl.loop(h * blocks, (h + 1) * blocks)
            def _(k):
                both = []
                for turn in range(2):
                    place = pl.ds(pl.multiple_of((2 * k + turn) * step, step), step)
                    both.append((partial[:, place] + torus_in[c % 2, :, place].astype(f32)) * dequant)
                gate, up = both
                cols = pl.ds(pl.multiple_of(k * step, step), step)
                hidden[:, cols] = (gate / (1.0 + jnp.exp(-gate)) * up).astype(bf16)

        for h in range(halves):
            across(c, h).wait_send()

    def lower(c):
        for h in range(pieces):
            @pl.loop(bounds[h], bounds[h + 1])
            def _(k):
                cols = tile_at(k)
                rows[c, :, cols] = dot(hidden[...], down_mat[:, cols]).astype(bf16)

            @pl.when(outer)
            def _():
                back(c, h).start()

    def cross(t, c):
        block = spread(t, c)
        rank = column(outer_ranks(block))[span:]
        scatter = jnp.where(places(tokens - span, pick, 1) == rank, 1.0, 0.0).astype(bf16)
        weight_in = column(row_of(block, here_in))[span:]
        weight_out = column(row_of(block, here_out))[span:]
        for h in range(pieces):
            back(c, h).wait_recv()
            for cols in piece_tiles(h):
                value = weight_out * dot(scatter, back_in[c, :, cols])
                value = value + weight_in * rows[c, pl.ds(span, tokens - span), cols].astype(f32)
                own_sum[c % 2, :, cols] = value[:span]
                cross_out[c % 2, :, cols] = value[span:].astype(bf16)
            cross_to_outer(c, h).start()
            cross_to_inner(c, h).start()

    def bring_home(t, c, h):
        weight = column(row_of(tables[here_out, t, c], here_in))[:span]
        for cols in piece_tiles(h):
            value = weight * rows[c, pl.ds(0, span), cols].astype(f32) + cross_in[c, :, cols].astype(f32)
            home_out[c % 2, :, cols] = value.astype(bf16)

    def own_part(t, c):
        weight = column(row_of(tables[node, t, c], node))[:span]

        @pl.loop(0, tiles)
        def _(k):
            cols = tile_at(k)
            own_sum[c % 2, :, cols] = weight * rows[c, pl.ds(span, span), cols].astype(f32)

    def finish(t, c, h):
        strip = pl.ds(pl.multiple_of(c * span, span), span)
        for cols in piece_tiles(h):
            value = stream[t, strip, cols].astype(f32) + own_sum[c % 2, :, cols]
            stream[t, strip, cols] = (value + cross_own[c, :, cols].astype(f32)).astype(bf16)

    def store_copy(t, c, h):
        strip = pl.ds(pl.multiple_of(c * span, span), span)
        return pltpu.make_async_copy(
            stream.at[t, strip, cut(h)], out_hbm.at[t, strip, cut(h)], store_sem.at[t, c, h]
        )

    barrier = pltpu.get_barrier_semaphore()

    def greet(target):
        pl.semaphore_signal(barrier, inc=1, device_id=target, device_id_type=MESH_ID)

    for k in range(1, 4):
        greet(at_node(lax.rem(node + k, 4)))
    greet((section, node, 1 - torus))

    @pl.when(section < sections - 1)
    def _():
        greet((section + 1, node, torus))

    @pl.when(section > 0)
    def _():
        greet((section - 1, node, torus))

    first_load = pltpu.make_async_copy(act_hbm, source, load_sem.at[0])
    first_load.start()
    next_load = pltpu.make_async_copy(next_hbm, arrived, load_sem.at[1])
    loads = [
        pltpu.make_async_copy(hbm, mat, load_sem.at[2 + i])
        for i, (hbm, mat) in enumerate(((gate_hbm, gate_mat), (up_hbm, up_mat), (down_hbm, down_mat)))
    ]
    table_copies = []
    for k in range(1, 4):
        other = lax.rem(node + k, 4)
        table_copies.append(
            pltpu.make_async_remote_copy(
                src_ref=tables.at[node], dst_ref=tables.at[node], send_sem=table_send.at[k - 1],
                recv_sem=table_recv.at[node], device_id=at_node(other), device_id_type=MESH_ID,
            )
        )
    index_copy = pltpu.make_async_remote_copy(
        src_ref=index.at[0], dst_ref=index_prev, send_sem=index_sem.at[0], recv_sem=index_sem.at[1],
        device_id=(section + 1, node, torus), device_id_type=MESH_ID,
    )

    def mate_copy(t):
        return pltpu.make_async_remote_copy(
            src_ref=peak_own.at[t], dst_ref=peak_mate.at[t], send_sem=mate_sem.at[0, t],
            recv_sem=mate_sem.at[1, t], device_id=(section, node, 1 - torus), device_id_type=MESH_ID,
        )

    def far_copy(t, k):
        return pltpu.make_async_remote_copy(
            src_ref=peak_pair.at[t], dst_ref=peak_far.at[t, node], send_sem=far_send.at[t, k - 1],
            recv_sem=far_recv.at[t, node], device_id=at_node(lax.rem(node + k, 4)), device_id_type=MESH_ID,
        )

    scale_tile[...] = jnp.broadcast_to(hist[...], scale_tile.shape)
    peak_own[...] = jnp.zeros_like(peak_own)
    for copy in loads:
        copy.start()
    sort_tokens(0)
    order[...] = jnp.where(places(tokens, tokens, 0) == index[0][0:1], 1.0, 0.0).astype(bf16)

    @pl.when(section == 0)
    def _():
        next_load.start()
        index_prev[...] = places(8, tokens, 1)

    first_load.wait()
    pl.semaphore_wait(
        barrier, 4 + jnp.where(section > 0, 1, 0) + jnp.where(section < sections - 1, 1, 0)
    )

    @pl.when(section < sections - 1)
    def _():
        index_copy.start()

    @pl.loop(0, 2)
    def _(t):
        @pl.when(t == 1)
        def _():
            @pl.when(section == 0)
            def _():
                next_load.wait()

        for h in range(pieces):
            @pl.when((t == 1) & (section > 0))
            def _():
                for c in range(CHUNKS):
                    to_next(c, h).wait_recv()

            prepare(t, 0, h)

            @pl.when(outer)
            def _():
                to_inner(0, h).start()

            @pl.when(inner)
            def _():
                own_copy(0, h).start()

            if h == 0:
                @pl.when(t == 0)
                def _():
                    sort_tokens(1)
                    make_table(0)
                    make_table(1)
                    for copy in table_copies:
                        copy.start()

            @pl.when(inner)
            def _():
                to_inner(0, h).wait_recv()
                relay(0, h).start()

        @pl.loop(1, jnp.where(outer, CHUNKS, 2))
        def _(c):
            for h in range(pieces):
                prepare(t, c, h)

                @pl.when(outer)
                def _():
                    to_inner(c, h).start()

                @pl.when(inner)
                def _():
                    own_copy(c, h).start()

        @pl.when(t == 0)
        def _():
            @pl.when(outer)
            def _():
                rows[:, 0:span, :] = jnp.zeros((CHUNKS, span, width), bf16)

            for k in range(1, 4):
                other = lax.rem(node + k, 4)
                pltpu.make_async_remote_copy(
                    src_ref=tables.at[node], dst_ref=tables.at[other], send_sem=table_send.at[k - 1],
                    recv_sem=table_recv.at[other], device_id=at_node(other), device_id_type=MESH_ID,
                ).wait_recv()

        @pl.loop(0, CHUNKS + 3)
        def _(it):
            @pl.when(it == 2)
            def _():
                mate_copy(t).start()

            @pl.when(it == 3)
            def _():
                mate_copy(t).wait_recv()
                peak_pair[t] = jnp.maximum(peak_own[t], peak_mate[t])
                for k in range(1, 4):
                    far_copy(t, k).start()

            @pl.when(it < CHUNKS)
            def _():
                @pl.when(inner)
                def _():
                    wait_all("wait_recv", lambda h: own_copy(it, h), lambda h: relay(it, h))

                    @pl.when((t > 0) | (it >= 2))
                    def _():
                        wait_all("wait_send", lambda h: picked(lax.rem(it + 2, CHUNKS), h))

                    select_for_outer(t, it)

                    @pl.when(it + 1 < CHUNKS)
                    def _():
                        for h in range(pieces):
                            to_inner(it + 1, h).wait_recv()
                            relay(it + 1, h).start()

                    @pl.when(it + 2 < CHUNKS)
                    def _():
                        for h in range(pieces):
                            prepare(t, it + 2, h)
                            own_copy(it + 2, h).start()

                @pl.when(outer)
                def _():
                    wait_all("wait_recv", lambda h: picked(it, h))

                @pl.when((t == 0) & (it == 0))
                def _():
                    for copy in loads:
                        copy.wait()

                project(it)

                @pl.when(inner)
                def _():
                    wait_all("wait_send", lambda h: own_copy(it, h), lambda h: relay(it, h))

                @pl.when(outer)
                def _():
                    wait_all("wait_send", lambda h: to_inner(it, h))

                activate(it)
                lower(it)

            @pl.when(inner & (it >= 2) & (it < CHUNKS + 2))
            def _():
                c = it - 2
                @pl.when((t > 0) | (c >= 2))
                def _():
                    last = lax.rem(c + 2, CHUNKS)
                    wait_all("wait_send", lambda h: cross_to_outer(last, h), lambda h: cross_to_inner(last, h))

                cross(t, c)

            @pl.when(it == CHUNKS + 2)
            def _():
                best = peak_pair[t]
                for k in range(1, 4):
                    other = lax.rem(node + k, 4)
                    pltpu.make_async_remote_copy(
                        src_ref=peak_pair.at[t], dst_ref=peak_far.at[t, other], send_sem=far_send.at[t, k - 1],
                        recv_sem=far_recv.at[t, other], device_id=at_node(other), device_id_type=MESH_ID,
                    ).wait_recv()
                    best = jnp.maximum(best, peak_far[t, other])
                scale_tile[...] = best
                peak_out[t] = best
                mate_copy(t).wait_send()
                for k in range(1, 4):
                    far_copy(t, k).wait_send()

                @pl.when(t == 0)
                def _():
                    @pl.when(section > 0)
                    def _():
                        index_copy.wait_recv()

                    now = jnp.where(places(tokens, tokens, 0) == index[1][0:1], 1.0, 0.0).astype(bf16)
                    was = jnp.where(places(tokens, tokens, 0) == index_prev[0:1], 1.0, 0.0).astype(bf16)
                    order[...] = lax.dot_general(
                        now, was, (((1,), (1,)), ((), ())), preferred_element_type=f32
                    ).astype(bf16)

            @pl.when(it >= 3)
            def _():
                c = it - 3

                @pl.when(inner & ((t > 0) | (c >= 2)))
                def _():
                    wait_all("wait_send", lambda h: home(lax.rem(c + 2, CHUNKS), h))

                @pl.when(outer)
                def _():
                    own_part(t, c)

                for h in range(pieces):
                    @pl.when(inner)
                    def _():
                        cross_to_outer(c, h).wait_recv()
                        bring_home(t, c, h)
                        home(c, h).start()
                        cross_to_inner(c, h).wait_recv()

                    @pl.when(outer)
                    def _():
                        home(c, h).wait_recv()

                    finish(t, c, h)

                    @pl.when((t == 0) & (section < sections - 1))
                    def _():
                        to_next(c, h).start()

                    store_copy(t, c, h).start()

        @pl.when(outer)
        def _():
            for c in range(CHUNKS):
                wait_all("wait_send", lambda h: back(c, h))

    @pl.when(inner)
    def _():
        for c in (CHUNKS - 2, CHUNKS - 1):
            wait_all(
                "wait_send", lambda h: picked(c, h), lambda h: cross_to_outer(c, h),
                lambda h: cross_to_inner(c, h), lambda h: home(c, h),
            )

    for copy in table_copies:
        copy.wait_send()

    @pl.when(section < sections - 1)
    def _():
        index_copy.wait_send()

        @pl.loop(0, CHUNKS)
        def _(c):
            wait_all("wait_send", lambda h: to_next(c, h))

    @pl.loop(0, CHUNKS)
    def _(c):
        wait_all("wait", lambda h: store_copy(0, c, h), lambda h: store_copy(1, c, h))


def restore_kernel(dealt, peaks, undo, out, peak_out):
    ticks = peak_out.shape[1]
    out[0] = dot(undo[0], dealt[0]).astype(jnp.bfloat16)
    lane = lax.broadcasted_iota(jnp.int32, (1, ticks), 1)
    line = jnp.zeros((1, ticks), jnp.float32)
    for t in range(ticks):
        line = jnp.where(lane == t, peaks[t, 0:1, 0:1], line)
    peak_out[...] = line


def fused_shards(act_in, next_in, routes, route_w, hist, gate_w, up_w, down_w):
    ticks, _, tokens, top = routes.shape
    width = act_in.shape[2]
    ffw = gate_w.shape[3]
    experts = lax.axis_size("node")
    span = tokens // CHUNKS
    capacity = 5 * tokens * top // (4 * experts)
    pick = 3 * ((capacity + (experts - 1) * (CHUNKS - 1)) // CHUNKS)
    pick = -(-pick // 16) * 16
    assert pick == 2 * span and span % 16 == 0 and width % TILE == 0 and ffw % 256 == 0
    by_rank = lambda value: value[:, 0].transpose(0, 2, 1)
    f32, bf16 = jnp.float32, jnp.bfloat16
    vmem, anywhere = pl.BlockSpec(memory_space=pltpu.VMEM), pl.BlockSpec(memory_space=pl.ANY)
    dma = pltpu.SemaphoreType.DMA
    tiles = width // TILE
    out, peaks, undo = pl.pallas_call(
        functools.partial(fused_kernel, lax.axis_size("section"), experts),
        out_shape=(
            jax.ShapeDtypeStruct((ticks, tokens, width), bf16),
            jax.ShapeDtypeStruct((ticks, 8, 128), f32),
            jax.ShapeDtypeStruct((ticks, tokens, tokens), bf16),
        ),
        in_specs=[anywhere, anywhere, vmem, vmem, vmem, anywhere, anywhere, anywhere],
        out_specs=(anywhere, vmem, vmem),
        scratch_shapes=[
            pltpu.VMEM((2, tokens, width), bf16),
            pltpu.VMEM((width, ffw), bf16),
            pltpu.VMEM((width, ffw), bf16),
            pltpu.VMEM((ffw, width), bf16),
            pltpu.VMEM((CHUNKS, tokens, width), bf16),
            pltpu.VMEM((2, tokens, width), bf16),
            pltpu.VMEM((2, pick, width), bf16),
            pltpu.VMEM((2, 2 * span, width), bf16),
            pltpu.VMEM((2, span, width), bf16),
            pltpu.VMEM((CHUNKS, pick, width), bf16),
            pltpu.VMEM((2, span, width), f32),
            pltpu.VMEM((CHUNKS, span, width), bf16),
            pltpu.VMEM((CHUNKS, span, width), bf16),
            pltpu.VMEM((tokens, 2 * ffw), bf16),
            pltpu.VMEM((2, tokens, 2 * ffw), bf16),
            pltpu.VMEM((tokens, 2 * ffw), f32),
            pltpu.VMEM((tokens, ffw), bf16),
            pltpu.VMEM((tokens, tokens), bf16),
            pltpu.VMEM((ticks, 8, tokens), f32),
            pltpu.VMEM((experts, ticks, CHUNKS, 2 * experts, 128), f32),
            pltpu.VMEM((8, tokens), f32),
            pltpu.VMEM((8, 128), f32),
            pltpu.VMEM((ticks, 8, 128), f32),
            pltpu.VMEM((ticks, 8, 128), f32),
            pltpu.VMEM((ticks, 8, 128), f32),
            pltpu.VMEM((ticks, experts, 8, 128), f32),
            dma((KINDS, CHUNKS, PIECES)),
            dma((KINDS, CHUNKS, PIECES)),
            dma((5,)),
            dma((ticks, CHUNKS, PIECES)),
            dma((experts - 1,)),
            dma((experts,)),
            dma((2,)),
            dma((2, ticks)),
            dma((ticks, experts - 1)),
            dma((ticks, experts)),
        ],
        compiler_params=pltpu.CompilerParams(
            collective_id=0, has_side_effects=True, vmem_limit_bytes=67043328
        ),
        name="fused_stack",
    )(
        act_in[0], next_in, by_rank(routes), by_rank(route_w), hist.reshape(1, 1), gate_w[0, 0], up_w[0, 0], down_w[0, 0]
    )
    block = width
    out, peaks = pl.pallas_call(
        restore_kernel,
        grid=(ticks, width // block),
        out_shape=(
            jax.ShapeDtypeStruct((ticks, tokens, width), bf16),
            jax.ShapeDtypeStruct((1, ticks), f32),
        ),
        in_specs=[
            pl.BlockSpec((1, tokens, block), lambda t, k: (t, 0, k)),
            pl.BlockSpec((ticks, 8, 128), lambda t, k: (0, 0, 0)),
            pl.BlockSpec((1, tokens, tokens), lambda t, k: (t, 0, 0)),
        ],
        out_specs=(
            pl.BlockSpec((1, tokens, block), lambda t, k: (t, 0, k)),
            pl.BlockSpec((1, ticks), lambda t, k: (0, 0)),
        ),
        name="restore_order",
    )(out, peaks, undo)
    return out[:, None], peaks


def solution(mesh):
    fused = mesh.shape["node"] == 4 and mesh.shape["torus"] == 2
    return jax.shard_map(
        fused_shards if fused else shards,
        mesh=mesh,
        in_specs=(
            P("section", "node", "torus"),
            P("node", "torus"),
            P(None, "section", "node", None),
            P(None, "section", "node", None),
            P("section"),
            P("section", "node", "torus", None),
            P("section", "node", "torus", None),
            P("section", "node", None, "torus"),
        ),
        out_specs=(P(None, "section", "node", "torus"), P("section", None)),
        check_vma=False,
    )
```

```python
import functools

import jax
import jax.numpy as jnp
from jax import lax
from jax.experimental import pallas as pl
from jax.experimental.pallas import tpu as pltpu
from jax.sharding import PartitionSpec as P

FP8_LIMIT = 448.0
MAX_CHUNKS = 4
DEPTH = 2


def shifted(value, axis, steps):
    count = lax.axis_size(axis)
    return lax.ppermute(value, axis, [(i, (i + steps) % count) for i in range(count)])


def swapped(value, axis):
    count = lax.axis_size(axis)
    return lax.ppermute(value, axis, [(i, i ^ 1) for i in range(count)])


def to_next_section(value):
    count = lax.axis_size("section")
    return lax.ppermute(value, "section", [(i, i + 1) for i in range(count - 1)])


def dot(left, right):
    return lax.dot_general(left, right, (((1,), (0,)), ((), ())), preferred_element_type=jnp.float32)


def torus_sum(value):
    if lax.axis_size("torus") == 2:
        return value + swapped(value.astype(jnp.bfloat16), "torus").astype(jnp.float32)
    return lax.psum(value, "torus")


def after(value, *earlier):
    return lax.optimization_barrier((value, *earlier))[0]


def ring_max(value, axis):
    count = lax.axis_size(axis)
    if count & (count - 1):
        return lax.pmax(value, axis)
    step = 1
    while step < count:
        value = jnp.maximum(value, shifted(value, axis, step))
        step *= 2
    return value


def routing_tables(expert_of, weight_of, capacity, n_node, me):
    tokens = expert_of.shape[0]
    pair = jnp.stack([me, me ^ 1]).astype(jnp.float32)
    named = expert_of[:, None, :] == pair[None, :, None]
    hit = jnp.any(named, axis=2)
    wgt = jnp.sum(jnp.where(named, weight_of[:, None, :], 0.0), axis=2)
    earlier = (jnp.arange(tokens)[:, None] > jnp.arange(tokens)[None, :]).astype(jnp.bfloat16)
    slots = jnp.arange(capacity, dtype=jnp.float32)
    rank = dot(earlier, hit.astype(jnp.bfloat16))
    chosen = (rank[:, :, None] == slots) & hit[:, :, None]
    table = chosen.astype(jnp.bfloat16).reshape(tokens, 2 * capacity)
    combine = jnp.where(chosen, wgt[:, :, None], 0.0).astype(jnp.bfloat16)
    return table.T, combine.reshape(tokens, 2 * capacity)


def shards(act_in, next_in, routes, route_w, hist, gate_w, up_w, down_w):
    tokens = act_in.shape[1]
    ticks = routes.shape[0]
    top = routes.shape[3]
    n_node = lax.axis_size("node")
    groups = n_node // 2
    capacity = 5 * tokens * top // (4 * n_node)
    half = groups * capacity
    gate_mat, up_mat, down_mat = gate_w[0, 0], up_w[0, 0], down_w[0, 0]
    width = gate_mat.shape[0]
    count = max(c for c in range(1, MAX_CHUNKS + 1) if width % (128 * c) == 0)
    size = width // count
    me = lax.axis_index("node")
    section_now = lax.axis_index("section")

    own_peak = jnp.max(jnp.abs(act_in[0])).astype(jnp.float32)
    packed = jnp.concatenate(
        [routes.astype(jnp.float32).reshape(-1), route_w.reshape(-1), jnp.full((128,), own_peak)]
    )
    amount = ticks * tokens * top
    known = [packed] + [shifted(packed, "node", -2 * k) for k in range(1, groups)]
    tables = []
    for tick in range(ticks):
        pairs = []
        for info in known:
            expert_of = info[:amount].reshape(ticks, tokens, top)[tick]
            weight_of = info[amount : 2 * amount].reshape(ticks, tokens, top)[tick]
            pairs.append(routing_tables(expert_of, weight_of, capacity, n_node, me))
        tables.append(tuple(zip(*pairs)))

    cuts = [slice(c * size, (c + 1) * size) for c in range(count)]
    streams = [act_in[0][:, cut] for cut in cuts]
    scale = hist[0]
    first_peak = known[0][-1:]
    for info in known[1:]:
        first_peak = jnp.maximum(first_peak, info[-1:])
    first_peak = ring_max(first_peak, "torus")
    first_peak = jnp.maximum(first_peak, swapped(first_peak, "node"))
    outputs, peaks = [], [first_peak[0]]
    for tick in range(ticks):
        select, combine = tables[tick]
        if tick > 0:
            streams = [
                lax.optimization_barrier(
                    jnp.where(section_now == 0, next_in[:, cut], to_next_section(outputs[-1][c]))
                )
                for c, cut in enumerate(cuts)
            ]
            scale = peaks[tick - 1]
        factor = FP8_LIMIT / scale
        dequant = scale / FP8_LIMIT
        gate = up = None
        sent = []
        for c, cut in enumerate(cuts):
            quantized = jnp.clip(
                streams[c].astype(jnp.float32) * factor, -FP8_LIMIT, FP8_LIMIT
            ).astype(jnp.bfloat16)
            if c >= DEPTH:
                quantized = after(quantized, sent[c - DEPTH], first_peak)
            if tick > 0 and c == count - 1:
                seen = [after(s, sent[0]) if sent else s for s in streams]
                here = [jnp.max(jnp.abs(s)).astype(jnp.float32).reshape(1) for s in seen]
                here = jnp.max(jnp.concatenate(here), keepdims=True)
                here = ring_max(ring_max(here, "torus"), "node")
                peaks.append(here[0])
                quantized = after(quantized, here)
            elif tick == 0:
                quantized = after(quantized, known[-1])
            held = [quantized] + [shifted(quantized, "node", -2 * k) for k in range(1, groups)]
            picked = [dot(select[k], held[k]).astype(jnp.bfloat16) for k in range(groups)]
            mine = jnp.concatenate([p[:capacity] for p in picked], axis=0)
            sent.append(jnp.concatenate([p[capacity:] for p in picked], axis=0))
            rows = jnp.concatenate([mine, swapped(sent[c], "node")], axis=0)
            gate_part = dot(rows, gate_mat[cut])
            up_part = dot(rows, up_mat[cut])
            gate = gate_part if gate is None else gate + gate_part
            up = up_part if up is None else up + up_part
        gate = torus_sum(gate) * dequant
        up = torus_sum(up) * dequant
        hidden = (jax.nn.silu(gate) * up).astype(jnp.bfloat16)
        layer, crossed = [], []
        for c, cut in enumerate(cuts):
            away_rows = hidden[half:]
            if c >= DEPTH:
                away_rows = after(away_rows, crossed[c - DEPTH])
            away = dot(away_rows, down_mat[:, cut]).astype(jnp.bfloat16)
            home_rows = after(hidden[:half], away)
            home = dot(home_rows, down_mat[:, cut]).astype(jnp.bfloat16)
            back = swapped(away, "node")
            branch = None
            for k in reversed(range(groups)):
                span = slice(k * capacity, (k + 1) * capacity)
                part = dot(combine[k], jnp.concatenate([home[span], back[span]], axis=0))
                if k > 0:
                    part = part.astype(jnp.bfloat16)
                    crossed = crossed + [part] if k == groups - 1 else crossed
                    part = shifted(part, "node", 2 * k).astype(jnp.float32)
                branch = part if branch is None else branch + part
            layer.append((streams[c].astype(jnp.float32) + branch).astype(jnp.bfloat16))
        outputs.append(layer)
    act_out = jnp.stack([jnp.concatenate(layer, axis=1) for layer in outputs])
    return act_out[:, None], jnp.stack(peaks)[None, :]


MESH_ID = pl.DeviceIdType.MESH
CHUNKS = 4
OWN, TO_INNER, RELAY, PICKED, BACK, CROSS_OUT, CROSS_IN, HOME, NEXT, TORUS, KINDS = range(11)
TILE = 512
PIECES = 2
HALVES = 2


def fused_kernel(
    sections, experts, act_hbm, next_hbm, routes, route_w, hist, gate_hbm, up_hbm, down_hbm,
    out_hbm, peak_out, undo,
    inputs, gate_mat, up_mat, down_mat, rows, stream, picked_out, cross_out, home_out,
    back_in, own_sum, cross_in, cross_own, torus_out, torus_in, partial, hidden, order,
    index, tables, index_prev, scale_tile, peak_own, peak_pair, peak_mate, peak_far,
    send, recv, load_sem, store_sem, table_send, table_recv, index_sem, mate_sem, far_send, far_recv,
):
    tokens, width = act_hbm.shape
    source, arrived = inputs.at[0], inputs.at[1]
    ffw = down_hbm.shape[0]
    span = tokens // CHUNKS
    pick = picked_out.shape[1]
    tiles = width // TILE
    halves, step = HALVES, 256
    blocks = ffw // step // halves
    section, node, torus = (lax.axis_index(a) for a in ("section", "node", "torus"))
    outer = (node == 0) | (node == 3)
    inner = jnp.logical_not(outer)
    side = node // 2
    mate = jnp.where(outer, 1 + side, 3 * side)
    facing = 2 - side
    far = 3 - 3 * side
    here_in, here_out = 1 + side, 3 * side
    f32, bf16 = jnp.float32, jnp.bfloat16

    pieces = min(PIECES, tiles)
    bounds = [-(-tiles * h // pieces) for h in range(pieces + 1)]

    def move(kind, c, src, dst, target, h=0):
        return pltpu.make_async_remote_copy(
            src_ref=src, dst_ref=dst, send_sem=send.at[kind, c, h], recv_sem=recv.at[kind, c, h],
            device_id=target, device_id_type=MESH_ID,
        )

    def cut(h):
        return slice(bounds[h] * TILE, bounds[h + 1] * TILE)

    def piece_tiles(h):
        return [slice(k * TILE, (k + 1) * TILE) for k in range(bounds[h], bounds[h + 1])]

    def at_node(n):
        return (section, n, torus)

    def part(c, first, h=None, count=1):
        return rows.at[c, pl.ds(first * span, count * span), slice(None) if h is None else cut(h)]

    def own_copy(c, h):
        return move(OWN, c, part(c, 1, h), part(c, 2, h), at_node(facing), h)

    def to_inner(c, h):
        return move(TO_INNER, c, part(c, 1, h), part(c, 0, h), at_node(mate), h)

    def relay(c, h):
        return move(RELAY, c, part(c, 0, h), part(c, 3, h), at_node(facing), h)

    def picked(c, h):
        return move(PICKED, c, picked_out.at[c % 2, :, cut(h)], part(c, 2, h, 2), at_node(mate), h)

    def back(c, h):
        return move(BACK, c, part(c, 2, h, 2), back_in.at[c, :, cut(h)], at_node(mate), h)

    def cross_to_outer(c, h):
        src = cross_out.at[c % 2, pl.ds(span, span), cut(h)]
        return move(CROSS_OUT, c, src, cross_in.at[c, :, cut(h)], at_node(facing), h)

    def cross_to_inner(c, h):
        src = cross_out.at[c % 2, pl.ds(0, span), cut(h)]
        return move(CROSS_IN, c, src, cross_own.at[c, :, cut(h)], at_node(facing), h)

    def home(c, h):
        return move(HOME, c, home_out.at[c % 2, :, cut(h)], cross_own.at[c, :, cut(h)], at_node(mate), h)

    def to_next(c, h):
        strip = pl.ds(c * span, span)
        src, dst = stream.at[0, strip, cut(h)], arrived.at[strip, cut(h)]
        return move(NEXT, c, src, dst, (section + 1, node, torus), h)

    def wait_all(end, *copies):
        for copy in copies:
            for h in range(pieces):
                getattr(copy(h), end)()

    def across(c, h):
        part_width = 2 * ffw // halves
        strip = slice(h * part_width, (h + 1) * part_width)
        return move(
            TORUS, c, torus_out.at[:, strip], torus_in.at[c % 2, :, strip], (section, node, 1 - torus), h
        )

    def eye(count):
        return lax.broadcasted_iota(jnp.int32, (count, count), 0) == lax.broadcasted_iota(
            jnp.int32, (count, count), 1
        )

    def column(row):
        count = row.shape[1]
        return jnp.sum(jnp.where(eye(count), row, 0.0), axis=1, keepdims=True)

    def row_of(block, number):
        at = lax.broadcasted_iota(jnp.int32, block.shape, 0) == number
        return jnp.sum(jnp.where(at, block, 0.0), axis=0, keepdims=True)

    def sort_tokens(t):
        picks = [routes[t, k : k + 1, :] for k in range(routes.shape[1])]
        low, high = functools.reduce(jnp.minimum, picks), functools.reduce(jnp.maximum, picks)
        lane = lax.broadcasted_iota(jnp.int32, (1, tokens), 1)
        key = ((low * experts + high) * tokens + lane).astype(f32)
        place = jnp.sum(jnp.where(column(key) < key, 1.0, 0.0), axis=0, keepdims=True).astype(jnp.int32)
        spot = (place & (CHUNKS - 1)) * span + (place >> (CHUNKS.bit_length() - 1))
        index[t] = jnp.broadcast_to(spot.astype(f32), (8, tokens))

    def make_table(t):
        at = jnp.where(column(index[t][0:1]) == places(tokens, tokens, 1), 1.0, 0.0).astype(bf16)
        undo[t] = at
        lines = []
        for weighted in (True, False):
            for e in range(experts):
                line = jnp.zeros((1, tokens), f32)
                for k in range(routes.shape[1]):
                    value = route_w[t, k : k + 1, :] if weighted else 1.0
                    line = line + jnp.where(routes[t, k : k + 1, :] == e, value, 0.0)
                lines.append(line)
        rest = jnp.concatenate(lines, axis=0)
        block = jnp.zeros_like(rest)
        for _ in range(3):
            term = rest.astype(bf16)
            block = block + dot(term, at)
            rest = rest - term.astype(f32)
        keep = lax.broadcasted_iota(jnp.int32, (2 * experts, 128), 1) < span
        for c in range(CHUNKS):
            first = c * span // 128 * 128
            half = block[:, first : first + 128]
            if c * span % 128:
                half = pltpu.roll(half, 128 - c * span % 128, 1)
            tables[node, t, c] = jnp.where(keep, half, 0.0)

    def spread(t, c):
        left = tables[here_out, t, c] + pltpu.roll(tables[here_in, t, c], span, 1)
        right = tables[facing, t, c] + pltpu.roll(tables[far, t, c], span, 1)
        return jnp.concatenate([left, right], axis=1)

    def outer_ranks(block):
        count = block.shape[1]
        lanes = lax.broadcasted_iota(jnp.int32, (1, count), 1)
        hit = jnp.where(lanes >= span, row_of(block, experts + here_out), 0.0)
        before = lax.broadcasted_iota(jnp.int32, (count, count), 0) < lax.broadcasted_iota(
            jnp.int32, (count, count), 1
        )
        wide = jnp.broadcast_to(hit, (8, count)).astype(bf16)
        rank = dot(wide, jnp.where(before, 1.0, 0.0).astype(bf16))[0:1]
        return jnp.where(hit > 0.0, rank, -1.0)

    def places(count, other, axis):
        return lax.broadcasted_iota(jnp.int32, (count, other), axis).astype(f32)

    def tile_at(k):
        return pl.ds(pl.multiple_of(k * TILE, TILE), TILE)

    def prepare(t, c, h):
        factor = FP8_LIMIT / scale_tile[0:1, 0:1]
        strip = pl.ds(pl.multiple_of(c * span, span), span)
        for cols in piece_tiles(h):
            value = dot(order[strip, :], inputs[t, :, cols])
            stream[t, strip, cols] = value.astype(bf16)
            top = jnp.max(jnp.max(jnp.abs(value), axis=0, keepdims=True), axis=1, keepdims=True)
            peak_own[t] = jnp.maximum(peak_own[t], top)
            rows[c, pl.ds(span, span), cols] = jnp.clip(
                value * factor, -FP8_LIMIT, FP8_LIMIT
            ).astype(bf16)

    def select_for_outer(t, c):
        rank = outer_ranks(spread(t, c))
        table_mat = jnp.where(places(pick, tokens, 0) == rank, 1.0, 0.0).astype(bf16)

        for h in range(pieces):
            @pl.loop(bounds[h], bounds[h + 1])
            def _(k):
                cols = tile_at(k)
                picked_out[c % 2, :, cols] = dot(table_mat, rows[c, :, cols]).astype(bf16)

            picked(c, h).start()

    def project(c):
        for h in range(halves):
            @pl.loop(h * blocks, (h + 1) * blocks)
            def _(k):
                cols = pl.ds(pl.multiple_of(k * step, step), step)
                for turn, mat in enumerate((gate_mat, up_mat)):
                    place = pl.ds(pl.multiple_of((2 * k + turn) * step, step), step)
                    value = dot(rows[c], mat[:, cols])
                    partial[:, place] = value
                    torus_out[:, place] = value.astype(bf16)

            across(c, h).start()

    def activate(c):
        dequant = scale_tile[0:1, 0:1] / FP8_LIMIT
        for h in range(halves):
            across(c, h).wait_recv()

            @pl.loop(h * blocks, (h + 1) * blocks)
            def _(k):
                both = []
                for turn in range(2):
                    place = pl.ds(pl.multiple_of((2 * k + turn) * step, step), step)
                    both.append((partial[:, place] + torus_in[c % 2, :, place].astype(f32)) * dequant)
                gate, up = both
                cols = pl.ds(pl.multiple_of(k * step, step), step)
                hidden[:, cols] = (gate / (1.0 + jnp.exp(-gate)) * up).astype(bf16)

        for h in range(halves):
            across(c, h).wait_send()

    def lower(c):
        for h in range(pieces):
            @pl.loop(bounds[h], bounds[h + 1])
            def _(k):
                cols = tile_at(k)
                rows[c, :, cols] = dot(hidden[...], down_mat[:, cols]).astype(bf16)

            @pl.when(outer)
            def _():
                back(c, h).start()

    def cross(t, c):
        block = spread(t, c)
        rank = column(outer_ranks(block))[span:]
        scatter = jnp.where(places(tokens - span, pick, 1) == rank, 1.0, 0.0).astype(bf16)
        weight_in = column(row_of(block, here_in))[span:]
        weight_out = column(row_of(block, here_out))[span:]
        for h in range(pieces):
            back(c, h).wait_recv()
            for cols in piece_tiles(h):
                value = weight_out * dot(scatter, back_in[c, :, cols])
                value = value + weight_in * rows[c, pl.ds(span, tokens - span), cols].astype(f32)
                own_sum[c % 2, :, cols] = value[:span]
                cross_out[c % 2, :, cols] = value[span:].astype(bf16)
            cross_to_outer(c, h).start()
            cross_to_inner(c, h).start()

    def bring_home(t, c, h):
        weight = column(row_of(tables[here_out, t, c], here_in))[:span]
        for cols in piece_tiles(h):
            value = weight * rows[c, pl.ds(0, span), cols].astype(f32) + cross_in[c, :, cols].astype(f32)
            home_out[c % 2, :, cols] = value.astype(bf16)

    def own_part(t, c):
        weight = column(row_of(tables[node, t, c], node))[:span]

        @pl.loop(0, tiles)
        def _(k):
            cols = tile_at(k)
            own_sum[c % 2, :, cols] = weight * rows[c, pl.ds(span, span), cols].astype(f32)

    def finish(t, c, h):
        strip = pl.ds(pl.multiple_of(c * span, span), span)
        for cols in piece_tiles(h):
            value = stream[t, strip, cols].astype(f32) + own_sum[c % 2, :, cols]
            stream[t, strip, cols] = (value + cross_own[c, :, cols].astype(f32)).astype(bf16)

    def store_copy(t, c, h):
        strip = pl.ds(pl.multiple_of(c * span, span), span)
        return pltpu.make_async_copy(
            stream.at[t, strip, cut(h)], out_hbm.at[t, strip, cut(h)], store_sem.at[t, c, h]
        )

    barrier = pltpu.get_barrier_semaphore()

    def greet(target):
        pl.semaphore_signal(barrier, inc=1, device_id=target, device_id_type=MESH_ID)

    for k in range(1, 4):
        greet(at_node(lax.rem(node + k, 4)))
    greet((section, node, 1 - torus))

    @pl.when(section < sections - 1)
    def _():
        greet((section + 1, node, torus))

    @pl.when(section > 0)
    def _():
        greet((section - 1, node, torus))

    first_load = pltpu.make_async_copy(act_hbm, source, load_sem.at[0])
    first_load.start()
    next_load = pltpu.make_async_copy(next_hbm, arrived, load_sem.at[1])
    loads = [
        pltpu.make_async_copy(hbm, mat, load_sem.at[2 + i])
        for i, (hbm, mat) in enumerate(((gate_hbm, gate_mat), (up_hbm, up_mat), (down_hbm, down_mat)))
    ]
    table_copies = []
    for k in range(1, 4):
        other = lax.rem(node + k, 4)
        table_copies.append(
            pltpu.make_async_remote_copy(
                src_ref=tables.at[node], dst_ref=tables.at[node], send_sem=table_send.at[k - 1],
                recv_sem=table_recv.at[node], device_id=at_node(other), device_id_type=MESH_ID,
            )
        )
    index_copy = pltpu.make_async_remote_copy(
        src_ref=index.at[0], dst_ref=index_prev, send_sem=index_sem.at[0], recv_sem=index_sem.at[1],
        device_id=(section + 1, node, torus), device_id_type=MESH_ID,
    )

    def mate_copy(t):
        return pltpu.make_async_remote_copy(
            src_ref=peak_own.at[t], dst_ref=peak_mate.at[t], send_sem=mate_sem.at[0, t],
            recv_sem=mate_sem.at[1, t], device_id=(section, node, 1 - torus), device_id_type=MESH_ID,
        )

    def far_copy(t, k):
        return pltpu.make_async_remote_copy(
            src_ref=peak_pair.at[t], dst_ref=peak_far.at[t, node], send_sem=far_send.at[t, k - 1],
            recv_sem=far_recv.at[t, node], device_id=at_node(lax.rem(node + k, 4)), device_id_type=MESH_ID,
        )

    scale_tile[...] = jnp.broadcast_to(hist[...], scale_tile.shape)
    peak_own[...] = jnp.zeros_like(peak_own)
    for copy in loads:
        copy.start()
    sort_tokens(0)
    order[...] = jnp.where(places(tokens, tokens, 0) == index[0][0:1], 1.0, 0.0).astype(bf16)

    @pl.when(section == 0)
    def _():
        next_load.start()
        index_prev[...] = places(8, tokens, 1)

    first_load.wait()
    pl.semaphore_wait(
        barrier, 4 + jnp.where(section > 0, 1, 0) + jnp.where(section < sections - 1, 1, 0)
    )

    @pl.when(section < sections - 1)
    def _():
        index_copy.start()

    def lead(t, h):
        @pl.when((t == 1) & (section > 0))
        def _():
            for c in range(CHUNKS):
                to_next(c, h).wait_recv()

        if h == 0:
            @pl.when((t == 1) & (section == 0))
            def _():
                next_load.wait()

        prepare(t, 0, h)

        @pl.when(outer)
        def _():
            to_inner(0, h).start()

        @pl.when(inner)
        def _():
            own_copy(0, h).start()

    @pl.loop(0, 2)
    def _(t):
        for h in range(pieces):
            if h == 0:
                @pl.when(t == 0)
                def _():
                    lead(0, 0)
            else:
                lead(t, h)

            if h == 0:
                @pl.when(t == 0)
                def _():
                    sort_tokens(1)
                    make_table(0)
                    make_table(1)
                    for copy in table_copies:
                        copy.start()

            @pl.when(inner)
            def _():
                to_inner(0, h).wait_recv()
                relay(0, h).start()

        @pl.loop(1, jnp.where(outer, CHUNKS, 2))
        def _(c):
            for h in range(pieces):
                prepare(t, c, h)

                @pl.when(outer)
                def _():
                    to_inner(c, h).start()

                @pl.when(inner)
                def _():
                    own_copy(c, h).start()

        @pl.when(t == 0)
        def _():
            @pl.when(outer)
            def _():
                rows[:, 0:span, :] = jnp.zeros((CHUNKS, span, width), bf16)

            for k in range(1, 4):
                other = lax.rem(node + k, 4)
                pltpu.make_async_remote_copy(
                    src_ref=tables.at[node], dst_ref=tables.at[other], send_sem=table_send.at[k - 1],
                    recv_sem=table_recv.at[other], device_id=at_node(other), device_id_type=MESH_ID,
                ).wait_recv()

        @pl.loop(0, CHUNKS + 3)
        def _(it):
            @pl.when(it == 2)
            def _():
                mate_copy(t).start()

            @pl.when(it == 3)
            def _():
                mate_copy(t).wait_recv()
                peak_pair[t] = jnp.maximum(peak_own[t], peak_mate[t])
                for k in range(1, 4):
                    far_copy(t, k).start()

            @pl.when(it < CHUNKS)
            def _():
                @pl.when(inner)
                def _():
                    wait_all("wait_recv", lambda h: own_copy(it, h), lambda h: relay(it, h))

                    @pl.when((t > 0) | (it >= 2))
                    def _():
                        wait_all("wait_send", lambda h: picked(lax.rem(it + 2, CHUNKS), h))

                    select_for_outer(t, it)

                    @pl.when(it + 1 < CHUNKS)
                    def _():
                        for h in range(pieces):
                            to_inner(it + 1, h).wait_recv()
                            relay(it + 1, h).start()

                    @pl.when(it + 2 < CHUNKS)
                    def _():
                        for h in range(pieces):
                            prepare(t, it + 2, h)
                            own_copy(it + 2, h).start()

                @pl.when(outer)
                def _():
                    wait_all("wait_recv", lambda h: picked(it, h))

                @pl.when((t == 0) & (it == 0))
                def _():
                    for copy in loads:
                        copy.wait()

                project(it)

                @pl.when(inner)
                def _():
                    wait_all("wait_send", lambda h: own_copy(it, h), lambda h: relay(it, h))

                @pl.when(outer)
                def _():
                    wait_all("wait_send", lambda h: to_inner(it, h))

                activate(it)
                lower(it)

            @pl.when(inner & (it >= 2) & (it < CHUNKS + 2))
            def _():
                c = it - 2
                @pl.when((t > 0) | (c >= 2))
                def _():
                    last = lax.rem(c + 2, CHUNKS)
                    wait_all("wait_send", lambda h: cross_to_outer(last, h), lambda h: cross_to_inner(last, h))

                cross(t, c)

            @pl.when(it == CHUNKS + 2)
            def _():
                best = peak_pair[t]
                for k in range(1, 4):
                    other = lax.rem(node + k, 4)
                    pltpu.make_async_remote_copy(
                        src_ref=peak_pair.at[t], dst_ref=peak_far.at[t, other], send_sem=far_send.at[t, k - 1],
                        recv_sem=far_recv.at[t, other], device_id=at_node(other), device_id_type=MESH_ID,
                    ).wait_recv()
                    best = jnp.maximum(best, peak_far[t, other])
                scale_tile[...] = best
                peak_out[t] = best
                mate_copy(t).wait_send()
                for k in range(1, 4):
                    far_copy(t, k).wait_send()

                @pl.when(t == 0)
                def _():
                    @pl.when(section > 0)
                    def _():
                        index_copy.wait_recv()

                    now = jnp.where(places(tokens, tokens, 0) == index[1][0:1], 1.0, 0.0).astype(bf16)
                    was = jnp.where(places(tokens, tokens, 0) == index_prev[0:1], 1.0, 0.0).astype(bf16)
                    order[...] = lax.dot_general(
                        now, was, (((1,), (1,)), ((), ())), preferred_element_type=f32
                    ).astype(bf16)

            @pl.when(it >= 3)
            def _():
                c = it - 3

                @pl.when(inner & ((t > 0) | (c >= 2)))
                def _():
                    wait_all("wait_send", lambda h: home(lax.rem(c + 2, CHUNKS), h))

                @pl.when(outer)
                def _():
                    own_part(t, c)

                for h in range(pieces):
                    @pl.when(inner)
                    def _():
                        cross_to_outer(c, h).wait_recv()
                        bring_home(t, c, h)
                        home(c, h).start()

                    if h == pieces - 1:
                        @pl.when((t == 0) & (c == CHUNKS - 1))
                        def _():
                            lead(1, 0)

                    @pl.when(inner)
                    def _():
                        cross_to_inner(c, h).wait_recv()

                    @pl.when(outer)
                    def _():
                        home(c, h).wait_recv()

                    finish(t, c, h)

                    @pl.when((t == 0) & (section < sections - 1))
                    def _():
                        to_next(c, h).start()

                    store_copy(t, c, h).start()

        @pl.when(outer)
        def _():
            for c in range(CHUNKS):
                wait_all("wait_send", lambda h: back(c, h))

    @pl.when(inner)
    def _():
        for c in (CHUNKS - 2, CHUNKS - 1):
            wait_all(
                "wait_send", lambda h: picked(c, h), lambda h: cross_to_outer(c, h),
                lambda h: cross_to_inner(c, h), lambda h: home(c, h),
            )

    for copy in table_copies:
        copy.wait_send()

    @pl.when(section < sections - 1)
    def _():
        index_copy.wait_send()

        @pl.loop(0, CHUNKS)
        def _(c):
            wait_all("wait_send", lambda h: to_next(c, h))

    @pl.loop(0, CHUNKS)
    def _(c):
        wait_all("wait", lambda h: store_copy(0, c, h), lambda h: store_copy(1, c, h))


def restore_kernel(dealt, peaks, undo, out, peak_out):
    ticks = peak_out.shape[1]
    out[0] = dot(undo[0], dealt[0]).astype(jnp.bfloat16)
    lane = lax.broadcasted_iota(jnp.int32, (1, ticks), 1)
    line = jnp.zeros((1, ticks), jnp.float32)
    for t in range(ticks):
        line = jnp.where(lane == t, peaks[t, 0:1, 0:1], line)
    peak_out[...] = line


def fused_shards(act_in, next_in, routes, route_w, hist, gate_w, up_w, down_w):
    ticks, _, tokens, top = routes.shape
    width = act_in.shape[2]
    ffw = gate_w.shape[3]
    experts = lax.axis_size("node")
    span = tokens // CHUNKS
    capacity = 5 * tokens * top // (4 * experts)
    pick = 3 * ((capacity + (experts - 1) * (CHUNKS - 1)) // CHUNKS)
    pick = -(-pick // 16) * 16
    assert pick == 2 * span and span % 16 == 0 and width % TILE == 0 and ffw % 256 == 0
    by_rank = lambda value: value[:, 0].transpose(0, 2, 1)
    f32, bf16 = jnp.float32, jnp.bfloat16
    vmem, anywhere = pl.BlockSpec(memory_space=pltpu.VMEM), pl.BlockSpec(memory_space=pl.ANY)
    dma = pltpu.SemaphoreType.DMA
    tiles = width // TILE
    out, peaks, undo = pl.pallas_call(
        functools.partial(fused_kernel, lax.axis_size("section"), experts),
        out_shape=(
            jax.ShapeDtypeStruct((ticks, tokens, width), bf16),
            jax.ShapeDtypeStruct((ticks, 8, 128), f32),
            jax.ShapeDtypeStruct((ticks, tokens, tokens), bf16),
        ),
        in_specs=[anywhere, anywhere, vmem, vmem, vmem, anywhere, anywhere, anywhere],
        out_specs=(anywhere, vmem, vmem),
        scratch_shapes=[
            pltpu.VMEM((2, tokens, width), bf16),
            pltpu.VMEM((width, ffw), bf16),
            pltpu.VMEM((width, ffw), bf16),
            pltpu.VMEM((ffw, width), bf16),
            pltpu.VMEM((CHUNKS, tokens, width), bf16),
            pltpu.VMEM((2, tokens, width), bf16),
            pltpu.VMEM((2, pick, width), bf16),
            pltpu.VMEM((2, 2 * span, width), bf16),
            pltpu.VMEM((2, span, width), bf16),
            pltpu.VMEM((CHUNKS, pick, width), bf16),
            pltpu.VMEM((2, span, width), f32),
            pltpu.VMEM((CHUNKS, span, width), bf16),
            pltpu.VMEM((CHUNKS, span, width), bf16),
            pltpu.VMEM((tokens, 2 * ffw), bf16),
            pltpu.VMEM((2, tokens, 2 * ffw), bf16),
            pltpu.VMEM((tokens, 2 * ffw), f32),
            pltpu.VMEM((tokens, ffw), bf16),
            pltpu.VMEM((tokens, tokens), bf16),
            pltpu.VMEM((ticks, 8, tokens), f32),
            pltpu.VMEM((experts, ticks, CHUNKS, 2 * experts, 128), f32),
            pltpu.VMEM((8, tokens), f32),
            pltpu.VMEM((8, 128), f32),
            pltpu.VMEM((ticks, 8, 128), f32),
            pltpu.VMEM((ticks, 8, 128), f32),
            pltpu.VMEM((ticks, 8, 128), f32),
            pltpu.VMEM((ticks, experts, 8, 128), f32),
            dma((KINDS, CHUNKS, PIECES)),
            dma((KINDS, CHUNKS, PIECES)),
            dma((5,)),
            dma((ticks, CHUNKS, PIECES)),
            dma((experts - 1,)),
            dma((experts,)),
            dma((2,)),
            dma((2, ticks)),
            dma((ticks, experts - 1)),
            dma((ticks, experts)),
        ],
        compiler_params=pltpu.CompilerParams(
            collective_id=0, has_side_effects=True, vmem_limit_bytes=67043328
        ),
        name="fused_stack",
    )(
        act_in[0], next_in, by_rank(routes), by_rank(route_w), hist.reshape(1, 1), gate_w[0, 0], up_w[0, 0], down_w[0, 0]
    )
    block = width
    out, peaks = pl.pallas_call(
        restore_kernel,
        grid=(ticks, width // block),
        out_shape=(
            jax.ShapeDtypeStruct((ticks, tokens, width), bf16),
            jax.ShapeDtypeStruct((1, ticks), f32),
        ),
        in_specs=[
            pl.BlockSpec((1, tokens, block), lambda t, k: (t, 0, k)),
            pl.BlockSpec((ticks, 8, 128), lambda t, k: (0, 0, 0)),
            pl.BlockSpec((1, tokens, tokens), lambda t, k: (t, 0, 0)),
        ],
        out_specs=(
            pl.BlockSpec((1, tokens, block), lambda t, k: (t, 0, k)),
            pl.BlockSpec((1, ticks), lambda t, k: (0, 0)),
        ),
        name="restore_order",
    )(out, peaks, undo)
    return out[:, None], peaks


def solution(mesh):
    fused = mesh.shape["node"] == 4 and mesh.shape["torus"] == 2
    return jax.shard_map(
        fused_shards if fused else shards,
        mesh=mesh,
        in_specs=(
            P("section", "node", "torus"),
            P("node", "torus"),
            P(None, "section", "node", None),
            P(None, "section", "node", None),
            P("section"),
            P("section", "node", "torus", None),
            P("section", "node", "torus", None),
            P("section", "node", None, "torus"),
        ),
        out_specs=(P(None, "section", "node", "torus"), P("section", None)),
        check_vma=False,
    )
```
